32 devices in a mesh: col: 8 (over z, x), bin: 4 (over y, core).
Axes of the slice: x: 2, y: 2, z: 4, core: 2. Of those that a mesh axis runs over, the one named last changes fastest.
Arguments:
- slope: float32 [131072], P('bin'), may hold values from -6 to 6
- curvature: float32 [131072], P('bin'), may hold values from -6 to 0
- target_mean: float32 [131072], P('bin'), may hold values from 0.15 to 0.85
- target_var: float32 [131072], P('bin'), may hold values from 0.06 to 0.12
- table: float32 [64, 512], P(None, 'col'), may hold values from -6 to 6
Outputs:
- species_mean: float32 [64, 131072], P('col')
- final_slope: float32 [131072], replicated
The draws below stay inside these ranges and needn't reach their ends.
All inputs are finite; a program needn't handle non-finite values.
Results may differ from the reference program's by a relative error of at most 0.0001.
Values sent between devices are 32-bit elements; how exact they have to be, the bound alone decides.
A program may use at most 64 MiB of HBM per device.

```python
import math
import jax
import jax.numpy as jnp
from jax import lax

CPTS = 512
SPECIES = 64
ITERS = 3
BINS = 131072


def block_levels(rng, shape, split, smallest, top_value):
    def one(axis_at, blocks):
        heights = jax.random.uniform(jax.random.fold_in(jax.random.fold_in(rng, 6), axis_at), (blocks,), jnp.float32, smallest / len(split), top_value / len(split))
        return jnp.repeat(jnp.exp(heights), shape[axis_at] // blocks).reshape((-1,) + (1,) * (len(shape) - axis_at - 1))

    factor_of = one(*split[0])
    for cut in split[1:]:
        factor_of = factor_of * one(*cut)
    return factor_of


def gaussian(key, shape, spread, bound, pieces=(), dtype=jnp.bfloat16):
    level = block_levels(key, shape, pieces, -0.22, 0.18) if pieces else 1.0
    result = jax.random.normal(key, shape, jnp.float32) * spread * level
    return jnp.minimum(jnp.maximum(result, -bound), bound).astype(dtype)


def setup_inputs(seed: int = 0) -> dict:
    key_list = jax.random.split(jax.random.key(seed), 6)
    return {
        "slope": jnp.clip(jax.random.uniform(key_list[0], (BINS,), jnp.float32, -6.0, 6.0) * block_levels(key_list[0], (BINS,), ((0, 4),), -0.4, 0.0), -6.0, 6.0),
        "curvature": jnp.clip(-6.0 + 6.0 * jax.random.uniform(key_list[1], (BINS,), jnp.float32) ** block_levels(key_list[1], (BINS,), ((0, 4),), -0.2, 0.2), -6.0, 0.0),
        "target_mean": jnp.clip(0.15 + 0.70000002 * jax.random.uniform(key_list[2], (BINS,), jnp.float32) ** block_levels(key_list[2], (BINS,), ((0, 4),), -0.2, 0.2), 0.15, 0.85),
        "target_var": jnp.clip(0.06 + 0.06 * jax.random.uniform(key_list[3], (BINS,), jnp.float32) ** block_levels(key_list[3], (BINS,), ((0, 4),), -0.2, 0.2), 0.06, 0.12),
        "table": gaussian(key_list[4], (SPECIES, CPTS), 1.0, 6.0, ((1, 8),), jnp.float32),
    }


def solve_block(items):
    slope, curvature, target_mean, target_var, table = items
    points = ((jnp.arange(CPTS).astype(jnp.float32) + 0.5) / CPTS)[:, None]
    lam = slope
    for step in range(ITERS):
        expo = jnp.exp(lam[None, :] * points + curvature[None, :] * points * points)
        partition = jnp.sum(expo, axis=0)
        moment = jnp.sum(points * expo, axis=0)
        lam = lam + (target_mean - moment / partition) / target_var
    expo = jnp.exp(lam[None, :] * points + curvature[None, :] * points * points)
    total = jnp.sum(expo, axis=0)
    weights = expo / total[None, :]
    values = jnp.dot(table, weights, precision=lax.Precision.HIGHEST, preferred_element_type=jnp.float32)
    return values, lam


def reference(slope, curvature, target_mean, target_var, table):
    block = math.gcd(BINS, 4096)
    count = BINS // block

    def one(items):
        return solve_block((items[0], items[1], items[2], items[3], table))

    stacked = (slope.reshape(count, block), curvature.reshape(count, block),
               target_mean.reshape(count, block), target_var.reshape(count, block))
    values, lam = lax.map(one, stacked)
    species_mean = jnp.transpose(values, (1, 0, 2)).reshape(SPECIES, BINS)
    return species_mean, lam.reshape(BINS)
```

```python
import functools
import math
import jax
import jax.numpy as jnp
from jax import lax
from jax.experimental import pallas as pl
from jax.experimental.pallas import tpu as pltpu
from jax.sharding import PartitionSpec as P

ITERS = 3
LANES = 128
LOG2E = math.log2(math.e)
MESH = pl.DeviceIdType.MESH
UNROLL = 32
STRIDE = 32
GROUP = 4
PARTS = 4
SINGLE = 2


def kernel(
    cols, bins, total_pts, rows,
    slope_hbm, curve_hbm, mean_hbm, var_hbm, placed_hbm,
    species, lam_ref,
    own, curve, placed, tab, lhs, lhs_own, consts, stage,
    isem, far, tsend, trecv, ksend, krecv, asend, arecv, bsend, brecv, rsend, rrecv,
    lsend, lrecv, msend, mrecv, ysend, yrecv, psend, precv,
):
    col = lax.axis_index("col")
    me = lax.axis_index("bin")
    core = lax.rem(me, 2)
    partner = me + 1 - 2 * core
    chips = bins // 2
    groups = cols // GROUP
    member = lax.rem(col, GROUP)
    group = col // GROUP
    sub = own.shape[1]
    width = sub * LANES
    part = width // PARTS
    part_rows = sub // PARTS
    singles = groups * SINGLE

    def other_chip(i):
        return lax.rem(me + 2 * i, bins)

    def peer(u, d):
        return lax.rem(group + u, groups) * GROUP + lax.rem(member + d, GROUP)

    def remote(src, dst, send, recv, c, b):
        return pltpu.make_async_remote_copy(
            src_ref=src, dst_ref=dst, send_sem=send, recv_sem=recv,
            device_id=(c, b), device_id_type=MESH,
        )

    def total_of(ref, send, recv):
        return remote(ref, ref, send, recv, col, partner)

    loads = [
        pltpu.make_async_copy(a.at[col], own.at[n], isem.at[n])
        for n, a in enumerate((slope_hbm, mean_hbm, var_hbm))
    ]
    loads.append(pltpu.make_async_copy(curve_hbm, curve.at[me], isem.at[3]))
    load_table = pltpu.make_async_copy(placed_hbm, placed, isem.at[4])
    load_table.start()
    for load in loads:
        load.start()

    def greet(sem, c, b):
        pl.semaphore_signal(sem, inc=1, device_id=(c, b), device_id_type=MESH)

    barrier = pltpu.get_barrier_semaphore()
    greet(barrier, col, partner)
    for d in range(1, GROUP):
        greet(barrier, peer(0, d), me)
    for i in range(1, chips):
        greet(barrier, col, other_chip(i))

    def greet_group(sem, g):
        for d in range(GROUP):
            greet(sem, g * GROUP + d, me)
        for i in range(1, chips):
            greet(sem, g * GROUP + member, other_chip(i))

    @pl.loop(group + 1, groups)
    def _(g):
        greet_group(barrier, g)

    each = GROUP + chips - 1
    h = 1.0 / total_pts
    wide = STRIDE * h
    first = (lax.broadcasted_iota(jnp.int32, consts.shape[1:], 0).astype(jnp.float32) + 0.5) * h
    consts[0] = first
    consts[1] = wide * (2.0 * first + wide)

    def table_copy(to):
        return remote(placed.at[pl.ds(to // GROUP * GROUP, GROUP)], tab.at[col], tsend.at[0], trecv.at[0], to, me)

    def curve_copy(i):
        at = curve.at[me, :, pl.ds(0, 2 * part_rows)]
        return remote(at, at, ksend.at[0], krecv.at[0], col, other_chip(i))

    def enter():
        pl.semaphore_wait(barrier, (group + 1) * each)

        @pl.loop(0, group)
        def _(g):
            greet_group(far, g)

        load_table.wait()

        @pl.loop(0, group)
        def _(g):
            for d in range(GROUP):
                table_copy(g * GROUP + d).start()

        for d in range(1, GROUP):
            table_copy(peer(0, d)).start()
        tab[col] = placed[pl.ds(group * GROUP, GROUP)]

    for load in loads:
        load.wait()

    curve2 = curve[me, col] * LOG2E
    target = own[1]
    var = own[2]
    lam = own[0]
    bend = jnp.exp2(curve2 * (2.0 * h * h))

    def newton(lam):
        lam2 = lam * LOG2E

        def begin(g):
            c = ((g * UNROLL).astype(jnp.float32) + 0.5) * h
            return jnp.exp2(c * (lam2 + curve2 * c)), jnp.exp2(h * (lam2 + curve2 * (2.0 * c + h)))

        def body(g, carry):
            total, mom, e, ratio = carry
            later = begin(g + 1)
            c = ((g * UNROLL).astype(jnp.float32) + 0.5) * h
            run = e
            runs = e
            for i in range(1, UNROLL):
                e = e * ratio
                if i < UNROLL - 1:
                    ratio = ratio * bend
                run = run + e
                runs = runs + run
            return total + run, mom + (c * run + h * (UNROLL * run - runs)), *later

        zero = jnp.zeros_like(lam)
        total, mom, _, _ = lax.fori_loop(0, total_pts // UNROLL, body, (zero, zero, *begin(jnp.int32(0))))
        return lam + (target - mom / total) / var

    @pl.when(group == groups - 1)
    def _():
        enter()

    lam = newton(lam)

    @pl.when(group < groups - 1)
    def _():
        enter()

    for i in range(1, chips):
        curve_copy(i).start()

    for step in range(1, ITERS):
        lam = newton(lam)
    lam_ref[me, col] = lam

    @pl.when(group < groups - 1)
    def _():
        pl.semaphore_wait(far, (groups - 1 - group) * each)

        @pl.loop(group + 1, groups)
        def _(g):
            for d in range(GROUP):
                table_copy(g * GROUP + d).start()

    def first_copy(i, u):
        at = lam_ref.at[me, col]
        return remote(at, at, asend.at[0], arecv.at[(chips - i) % chips, lax.rem(groups - u, groups)], peer(u, 0), other_chip(i))

    def first_arrival(i, u):
        b, j = other_chip(i), peer(u, 0)
        at = lam_ref.at[b, j]
        return remote(at, at, asend.at[0], arecv.at[i, u], j, b)

    for i in range(1, chips):
        first_copy(i, 0).start()

    @pl.loop(1, groups)
    def _(u):
        for i in range(chips):
            first_copy(i, u).start()

    total_of(tab.at[pl.ds(0, cols - 1)], tsend.at[0], trecv.at[0]).wait_recv()

    def halves(full):
        high = full.astype(jnp.bfloat16).astype(jnp.float32)
        return high, full - high

    def twice(pieces):
        whole = jnp.concatenate([*pieces, jnp.ones((16, total_pts), jnp.float32)], axis=0).astype(jnp.bfloat16)
        return jnp.concatenate([whole, whole], axis=1)

    span = GROUP * rows
    pad = (lhs_own.shape[0] - 16) // 2
    lhs[...] = twice(halves(jnp.concatenate(
        [jnp.concatenate([tab[t, n] for n in range(GROUP)], axis=0) for t in range(cols)], axis=1
    )))
    mine = jnp.concatenate([tab[t, member] for t in range(cols)], axis=1)
    if pad > rows:
        mine = jnp.concatenate([mine, jnp.zeros((pad - rows, total_pts), jnp.float32)], axis=0)
    lhs_own[...] = twice(halves(mine))

    def lanes(q):
        return pl.ds(pl.multiple_of(q * part, LANES), part)

    def weighted(left, b, j, r):
        lam_t = jnp.concatenate([lam_ref[b, j, pl.ds(r + n, 1)] for n in range(2)], axis=1) * LOG2E
        cur_t = jnp.concatenate([curve[b, j, pl.ds(r + n, 1)] for n in range(2)], axis=1) * LOG2E
        c = consts[0]
        e = jnp.exp2(c * (lam_t + cur_t * c))
        ratio = jnp.exp2(wide * lam_t + cur_t * consts[1])
        turn = jnp.broadcast_to(jnp.exp2(cur_t * (2.0 * wide * wide)), e.shape)
        highs, lows = [], []
        steps = total_pts // STRIDE
        for m in range(steps):
            e_hi = e.astype(jnp.bfloat16)
            highs.append(e_hi)
            lows.append((e - e_hi.astype(jnp.float32)).astype(jnp.bfloat16))
            if m < steps - 1:
                e = e * ratio
            if m < steps - 2:
                ratio = ratio * turn
        return jnp.dot(left[...], jnp.concatenate(highs + lows, axis=0), preferred_element_type=jnp.float32)

    def compute(item, b, j, q):
        for t in range(part_rows // 2):
            acc = weighted(lhs, b, j, q * part_rows + t * 2)
            inv = 1.0 / acc[2 * span:2 * span + 8]
            at = pl.ds(t * 2 * LANES, 2 * LANES)
            for n in range(GROUP):
                value = acc[n * rows:(n + 1) * rows] + acc[span + n * rows:span + (n + 1) * rows]
                stage[item, n, :, at] = value * inv[:rows]
        species[b, j, :, lanes(q)] = stage[item, member]

    def local(b, j):
        for t in range(part_rows // 2):
            acc = weighted(lhs_own, b, j, t * 2)
            inv = 1.0 / acc[2 * pad:2 * pad + 8]
            species[b, j, :, pl.ds(t * 2 * LANES, 2 * LANES)] = (acc[:rows] + acc[pad:pad + rows]) * inv[:rows]
        hand_on(b, j, 0)

    def member_copy(item, d, b, j, q):
        to = lax.rem(member + d, GROUP)
        return remote(stage.at[item, to], species.at[b, j, :, lanes(q)], msend.at[0], mrecv.at[item, member], group * GROUP + to, me)

    def member_arrival(item, d, b, j, q):
        at = species.at[b, j, :, lanes(q)]
        return remote(at, at, msend.at[0], mrecv.at[item, lax.rem(member + d, GROUP)], col, partner)

    def y_copy(i, j, q):
        at = species.at[me, j, :, lanes(q)]
        return remote(at, at, ysend.at[0], yrecv.at[chips - 1 - i, j, q - (PARTS - SINGLE)], col, other_chip(i))

    def y_arrival(i, j, q):
        at = species.at[other_chip(i), j, :, lanes(q)]
        return remote(at, at, ysend.at[0], yrecv.at[i - 1, j, q - (PARTS - SINGLE)], col, other_chip(i))

    def hand_on(b, j, q):
        at = species.at[b, j, :, lanes(q)]
        remote(at, at, psend.at[0], precv.at[0], col, partner).start()

    def second_copy(u, i, d):
        at = lam_ref.at[other_chip(i), peer(u, 0), pl.ds(0, part_rows)]
        return remote(at, at, bsend.at[0], brecv.at[u, member], peer(0, d), me)

    def second_arrival(u, d):
        at = lam_ref.at[pl.ds(0, chips), 0, pl.ds(0, part_rows)]
        return remote(at, at, bsend.at[0], brecv.at[u, lax.rem(member + d, GROUP)], col, partner)

    def rest_copy(u, i, d):
        at = lam_ref.at[other_chip(i), peer(u, 0), pl.ds(part_rows, sub - part_rows)]
        return remote(at, at, rsend.at[0], rrecv.at[0], peer(0, d), me)

    def single_item(u, k):
        item = u * SINGLE + k
        q = PARTS - SINGLE + k
        j = peer(u, 0)
        compute(item, me, j, q)
        for d in range(1, GROUP):
            member_copy(item, d, me, j, q).start()
        for i in range(1, chips):
            y_copy(i, j, q).start()
        hand_on(me, j, q)

    def double_item(u, i):
        item = singles + u * chips + i
        b, j = other_chip(i), peer(u, 0)
        compute(item, b, j, 1)
        for d in range(1, GROUP):
            member_copy(item, d, b, j, 1).start()
        hand_on(b, j, 1)

    @pl.loop(0, groups)
    def _(u):
        @pl.when(u > 0)
        def _():
            first_arrival(0, u).wait_recv()

        @pl.loop(0, SINGLE)
        def _(k):
            single_item(u, k)

        for i in range(1, chips):
            first_arrival(i, u).wait_recv()

        @pl.when(u == 0)
        def _():
            total_of(curve.at[pl.ds(0, chips - 1), :, pl.ds(0, 2 * part_rows)], ksend.at[0], krecv.at[0]).wait_recv()

        for i in range(chips):
            for d in range(1, GROUP):
                second_copy(u, i, d).start()

        @pl.loop(0, chips)
        def _(i):
            double_item(u, i)
            local(other_chip(i), peer(u, 0))

        for k in range(SINGLE):
            for d in range(1, GROUP):
                q = PARTS - SINGLE + k
                j = peer(u, d)
                member_arrival(u * SINGLE + k, d, me, j, q).wait_recv()
                for i in range(1, chips):
                    y_copy(i, j, q).start()
                hand_on(me, j, q)

    @pl.loop(0, groups)
    def _(u):
        for i in range(chips):
            for d in range(1, GROUP):
                rest_copy(u, i, d).start()

    def y_arrivals(u, d):
        for k in range(SINGLE):
            for i in range(1, chips):
                q = PARTS - SINGLE + k
                y_arrival(i, peer(u, d), q).wait_recv()
                hand_on(other_chip(i), peer(u, d), q)

    @pl.loop(0, groups)
    def _(u):
        @pl.loop(1, GROUP)
        def _(d):
            second_arrival(u, d).wait_recv()

            @pl.loop(0, chips)
            def _(i):
                b, j = other_chip(i), peer(u, d)
                local(b, j)
                member_arrival(singles + u * chips + i, d, b, j, 1).wait_recv()
                hand_on(b, j, 1)

            @pl.when(u > 0)
            def _():
                y_arrivals(u - 1, d)

    total_of(lam_ref.at[pl.ds(0, chips), pl.ds(0, (GROUP - 1) * groups), pl.ds(part_rows, sub - part_rows)], rsend.at[0], rrecv.at[0]).wait_recv()
    for i in range(chips):
        at = lam_ref.at[other_chip(i)]
        remote(at, at, lsend.at[0], lrecv.at[0], col, partner).start()

    @pl.loop(0, groups)
    def _(u):
        y_arrivals(u, 0)

    @pl.loop(1, GROUP)
    def _(d):
        y_arrivals(groups - 1, d)

    total_of(tab.at[pl.ds(0, cols - 1)], tsend.at[0], trecv.at[0]).wait_send()
    total_of(curve.at[pl.ds(0, chips - 1), :, pl.ds(0, 2 * part_rows)], ksend.at[0], krecv.at[0]).wait_send()
    total_of(lam_ref.at[0, pl.ds(0, chips * groups - 1)], asend.at[0], lrecv.at[0]).wait_send()
    spread = pl.ds(0, (GROUP - 1) * groups)
    total_of(lam_ref.at[pl.ds(0, chips), spread, pl.ds(0, part_rows)], bsend.at[0], lrecv.at[0]).wait_send()
    total_of(lam_ref.at[pl.ds(0, chips), spread, pl.ds(part_rows, sub - part_rows)], rsend.at[0], lrecv.at[0]).wait_send()
    total_of(stage.at[:, pl.ds(0, GROUP - 1)], msend.at[0], precv.at[0]).wait_send()
    total_of(species.at[pl.ds(0, chips - 1), :, :, pl.ds(0, SINGLE * part)], ysend.at[0], precv.at[0]).wait_send()
    total_of(lam_ref.at[pl.ds(0, chips)], lsend.at[0], lrecv.at[0]).wait()
    total_of(species.at[pl.ds(0, chips)], psend.at[0], precv.at[0]).wait()


def write_kernel(species, lam, out_ref, lam_out, sem):
    bins, cols, _, width = species.shape
    for b in range(bins):
        for j in range(cols):
            pltpu.make_async_copy(species.at[b, j], out_ref.at[:, pl.ds((b * cols + j) * width, width)], sem.at[0]).start()
    keep = pltpu.make_async_copy(lam, lam_out, sem.at[1])
    keep.start()
    pltpu.make_async_copy(out_ref, out_ref, sem.at[0]).wait()
    keep.wait()


def per_device(slope, curvature, target_mean, target_var, table):
    cols = lax.axis_size("col")
    bins = lax.axis_size("bin")
    all_species, pts = table.shape
    rows = all_species // cols
    pad = -(-rows // 8) * 8
    total_pts = pts * cols
    per_shard = slope.shape[0]
    sub = per_shard // cols // LANES
    width = sub * LANES
    chips = bins // 2
    groups = cols // GROUP
    items = groups * (SINGLE + chips)

    def blocks(a):
        return a.reshape(cols, sub, LANES)

    placed = table.reshape(cols, rows, pts)
    vmem = pl.BlockSpec(memory_space=pltpu.VMEM)
    hbm = pl.BlockSpec(memory_space=pltpu.HBM)
    dma = pltpu.SemaphoreType.DMA
    one = dma((1,))
    species, lam = pl.pallas_call(
        functools.partial(kernel, cols, bins, total_pts, rows),
        out_shape=(
            jax.ShapeDtypeStruct((bins, cols, rows, width), jnp.float32),
            jax.ShapeDtypeStruct((bins, cols, sub, LANES), jnp.float32),
        ),
        in_specs=[hbm] * 5,
        out_specs=(vmem, vmem),
        scratch_shapes=[
            pltpu.VMEM((3, sub, LANES), jnp.float32),
            pltpu.VMEM((bins, cols, sub, LANES), jnp.float32),
            pltpu.VMEM((cols, rows, pts), jnp.float32),
            pltpu.VMEM((cols, GROUP, rows, pts), jnp.float32),
            pltpu.VMEM((2 * GROUP * rows + 16, 2 * total_pts), jnp.bfloat16),
            pltpu.VMEM((2 * pad + 16, 2 * total_pts), jnp.bfloat16),
            pltpu.VMEM((2, STRIDE, 2 * LANES), jnp.float32),
            pltpu.VMEM((items, GROUP, rows, width // PARTS), jnp.float32),
            dma((5,)), pltpu.SemaphoreType.REGULAR,
            one, one, one, one, one, dma((chips, groups)),
            one, dma((groups, GROUP)), one, one,
            one, one, one, dma((items, GROUP)),
            one, dma((chips - 1, cols, SINGLE)), one, one,
        ],
        compiler_params=pltpu.CompilerParams(collective_id=0, has_side_effects=True, vmem_limit_bytes=24 << 20),
    )(*[
        pltpu.with_memory_space_constraint(a, pltpu.HBM)
        for a in (blocks(slope), blocks(curvature), blocks(target_mean), blocks(target_var), placed)
    ])
    species_mean, lam = pl.pallas_call(
        write_kernel,
        out_shape=(
            jax.ShapeDtypeStruct((rows, per_shard * bins), jnp.float32),
            jax.ShapeDtypeStruct((bins, cols, sub, LANES), jnp.float32),
        ),
        in_specs=[vmem, vmem],
        out_specs=(hbm, hbm),
        scratch_shapes=[dma((2,))],
        compiler_params=pltpu.CompilerParams(vmem_limit_bytes=4 << 20),
    )(species, lam)
    return species_mean, lam.reshape(-1)


def solution(mesh):
    placed = (P("bin"), P("bin"), P("bin"), P("bin"), P(None, "col"))
    return jax.shard_map(
        per_device, mesh=mesh, in_specs=placed, out_specs=(P("col", None), P()), check_vma=False
    )
```

```python
import functools
import math
import jax
import jax.numpy as jnp
from jax import lax
from jax.experimental import pallas as pl
from jax.experimental.pallas import tpu as pltpu
from jax.sharding import PartitionSpec as P

ITERS = 3
LANES = 128
LOG2E = math.log2(math.e)
MESH = pl.DeviceIdType.MESH
UNROLL = 32
STRIDE = 32
DEPTH = 256
GROUP = 4
PARTS = 4
SINGLE = 2


def kernel(
    cols, bins, total_pts, rows,
    slope_hbm, curve_hbm, mean_hbm, var_hbm, placed_hbm,
    species, lam_ref,
    own, curve, placed, packed, tab, lhs, lhs_own, consts, stage,
    isem, far, tsend, trecv, ksend, krecv, asend, arecv, bsend, brecv,
    lsend, lrecv, msend, mrecv, ysend, yrecv, psend, precv,
    sums,
):
    col = lax.axis_index("col")
    me = lax.axis_index("bin")
    core = lax.rem(me, 2)
    partner = me + 1 - 2 * core
    chips = bins // 2
    groups = cols // GROUP
    member = lax.rem(col, GROUP)
    group = col // GROUP
    last = groups - 1
    sub = own.shape[1]
    width = sub * LANES
    part = width // PARTS
    part_rows = sub // PARTS
    pts = total_pts // cols
    side = packed.shape[3] // pts
    per = SINGLE + chips
    blocks = part_rows // 2
    lag = blocks % 2 == 0
    sums_group, sums_own = sums

    def other_chip(i):
        return lax.rem(me + 2 * i, bins)

    def peer(u, d):
        return lax.rem(group + u, groups) * GROUP + lax.rem(member + d, GROUP)

    def remote(src, dst, send, recv, c, b):
        return pltpu.make_async_remote_copy(
            src_ref=src, dst_ref=dst, send_sem=send, recv_sem=recv,
            device_id=(c, b), device_id_type=MESH,
        )

    def total_of(ref, send, recv):
        return remote(ref, ref, send, recv, col, partner)

    def greet(sem, c, b):
        pl.semaphore_signal(sem, inc=1, device_id=(c, b), device_id_type=MESH)

    barrier = pltpu.get_barrier_semaphore()
    greet(barrier, col, partner)
    for d in range(1, GROUP):
        greet(barrier, peer(0, d), me)
    for i in range(1, chips):
        greet(barrier, col, other_chip(i))

    def greet_group(sem, g):
        for d in range(GROUP):
            greet(sem, g * GROUP + d, me)
        for i in range(1, chips):
            greet(sem, g * GROUP + member, other_chip(i))

    @pl.loop(group + 1, groups)
    def _(g):
        greet_group(barrier, g)

    load_table = pltpu.make_async_copy(placed_hbm, placed, isem.at[4])
    load_table.start()
    loads = [
        pltpu.make_async_copy(a.at[col], own.at[n], isem.at[n])
        for n, a in enumerate((slope_hbm, mean_hbm, var_hbm))
    ]
    loads.append(pltpu.make_async_copy(curve_hbm, curve.at[me], isem.at[3]))
    for load in loads:
        load.start()

    for pair in (*sums_group, *sums_own):
        for acc in pair:
            pltpu.matmul_pop(acc)

    each = GROUP + chips - 1
    h = 1.0 / total_pts
    wide = STRIDE * h
    first = (lax.broadcasted_iota(jnp.int32, consts.shape[1:], 0).astype(jnp.float32) + 0.5) * h
    consts[0] = first
    consts[1] = wide * (2.0 * first + wide)

    load_table.wait()
    for g in range(groups):
        for p in range(GROUP // side):
            packed[g, p] = jnp.concatenate([placed[g * GROUP + p * side + n] for n in range(side)], axis=1)

    def table_copy(to):
        return remote(packed.at[to // GROUP], tab.at[col], tsend.at[0], trecv.at[0], to, me)

    def curve_copy(i):
        at = curve.at[me, :, pl.ds(0, 2 * part_rows)]
        return remote(at, at, ksend.at[0], krecv.at[0], col, other_chip(i))

    def enter():
        pl.semaphore_wait(barrier, (group + 1) * each)

        @pl.loop(0, group)
        def _(g):
            greet_group(far, g)

        @pl.loop(0, group)
        def _(g):
            for d in range(GROUP):
                table_copy(g * GROUP + d).start()

        for d in range(1, GROUP):
            table_copy(peer(0, d)).start()
        tab[col] = packed[group]

    for load in loads:
        load.wait()

    @pl.when(group == last)
    def _():
        enter()
        for i in range(1, chips):
            curve_copy(i).start()

    curve2 = curve[me, col] * LOG2E
    target = own[1]
    var = own[2]
    lam = own[0]
    bend = jnp.exp2(curve2 * (2.0 * h * h))

    def newton(lam):
        lam2 = lam * LOG2E

        def begin(g):
            c = ((g * UNROLL).astype(jnp.float32) + 0.5) * h
            return jnp.exp2(c * (lam2 + curve2 * c)), jnp.exp2(h * (lam2 + curve2 * (2.0 * c + h)))

        def body(g, carry):
            total, mom, e, ratio = carry
            later = begin(g + 1)
            c = ((g * UNROLL).astype(jnp.float32) + 0.5) * h
            run = e
            runs = e
            for i in range(1, UNROLL):
                e = e * ratio
                if i < UNROLL - 1:
                    ratio = ratio * bend
                run = run + e
                runs = runs + run
            return total + run, mom + (c * run + h * (UNROLL * run - runs)), *later

        zero = jnp.zeros_like(lam)
        total, mom, _, _ = lax.fori_loop(0, total_pts // UNROLL, body, (zero, zero, *begin(jnp.int32(0))))
        return lam + (target - mom / total) / var

    for step in range(ITERS):
        lam = newton(lam)
    lam_ref[me, col] = lam

    @pl.when(group < last)
    def _():
        enter()

    def first_copy(i, u):
        at = lam_ref.at[me, col]
        return remote(at, at, asend.at[0], arecv.at[(chips - i) % chips, lax.rem(groups - u, groups)], peer(u, 0), other_chip(i))

    def first_arrival(i, u):
        b, j = other_chip(i), peer(u, 0)
        at = lam_ref.at[b, j]
        return remote(at, at, asend.at[0], arecv.at[i, u], j, b)

    def second_copy(u, i, d):
        at = lam_ref.at[other_chip(i), peer(u, 0)]
        return remote(at, at, bsend.at[0], brecv.at[u, member], peer(0, d), me)

    def second_arrival(u, d):
        at = lam_ref.at[pl.ds(0, chips), 0]
        return remote(at, at, bsend.at[0], brecv.at[u, lax.rem(member + d, GROUP)], col, partner)

    for i in range(1, chips):
        first_copy(i, 0).start()
    for d in range(1, GROUP):
        second_copy(0, 0, d).start()

    @pl.when(group < last)
    def _():
        for i in range(1, chips):
            curve_copy(i).start()
        pl.semaphore_wait(far, (last - group) * each)

        @pl.loop(group + 1, groups)
        def _(g):
            for d in range(GROUP):
                table_copy(g * GROUP + d).start()

    @pl.loop(1, groups)
    def _(u):
        for i in range(chips):
            first_copy(i, u).start()

    total_of(tab.at[pl.ds(0, cols - 1)], tsend.at[0], trecv.at[0]).wait_recv()

    def split(full):
        high = full.astype(jnp.bfloat16).astype(jnp.float32)
        return jnp.concatenate([high, full - high, jnp.ones((16, total_pts), jnp.float32)], axis=0).astype(jnp.bfloat16)

    def gathered(n):
        return jnp.concatenate([tab[t, n // side][:, n % side * pts:(n % side + 1) * pts] for t in range(cols)], axis=1)

    span = GROUP * rows
    pad = (lhs_own.shape[0] - 16) // 2
    every = [gathered(n) for n in range(GROUP)]
    lhs[...] = split(jnp.concatenate(every, axis=0))
    mine = every[0]
    for n in range(1, GROUP):
        mine = jnp.where(member == n, every[n], mine)
    if pad > rows:
        mine = jnp.concatenate([mine, jnp.zeros((pad - rows, total_pts), jnp.float32)], axis=0)
    lhs_own[...] = split(mine)

    def lanes(q):
        return pl.ds(pl.multiple_of(q * part, LANES), part)

    def push(left, accs, b, j, r):
        lam_t = jnp.concatenate([lam_ref[b, j, pl.ds(r + n, 1)] for n in range(2)], axis=1) * LOG2E
        cur_t = jnp.concatenate([curve[b, j, pl.ds(r + n, 1)] for n in range(2)], axis=1) * LOG2E
        c = consts[0]
        e = jnp.exp2(c * (lam_t + cur_t * c))
        ratio = jnp.exp2(wide * lam_t + cur_t * consts[1])
        turn = jnp.broadcast_to(jnp.exp2(cur_t * (2.0 * wide * wide)), e.shape)
        steps = DEPTH // STRIDE
        tiles = total_pts // DEPTH
        for n in range(tiles):
            highs, lows = [], []
            for m in range(steps):
                e_hi = e.astype(jnp.bfloat16)
                highs.append(e_hi)
                lows.append((e - e_hi.astype(jnp.float32)).astype(jnp.bfloat16))
                if n < tiles - 1 or m < steps - 1:
                    e = e * ratio
                    ratio = ratio * turn
            for q, pieces in enumerate((highs, lows)):
                pltpu.matmul_push_rhs(jnp.concatenate(pieces, axis=0), n % 2, q)
            piece = left[:, n * DEPTH:(n + 1) * DEPTH]
            for acc in accs:
                pltpu.matmul_acc_lhs(acc, piece, load_staged_rhs=n % 2)

    def pick(t):
        return (blocks - t) % 2

    def at_block(t):
        return pl.ds(t * 2 * LANES, 2 * LANES)

    def run(start, done, sent, before=None):
        for t in range(blocks):
            start(t)
            if t > 0:
                done(t - 1)
            elif before is not None:
                before()
        if not lag:
            done(blocks - 1)
            sent()

    def close(done, sent):
        if lag:
            done(blocks - 1)
            sent()

    def hand_on(b, j, q):
        at = species.at[b, j, :, lanes(q)]
        remote(at, at, psend.at[0], precv.at[0], col, partner).start()

    def member_copy(item, d, b, j, q):
        to = lax.rem(member + d, GROUP)
        return remote(stage.at[item, to], species.at[b, j, :, lanes(q)], msend.at[0], mrecv.at[item], group * GROUP + to, me)

    def member_arrivals(item):
        total_of(species.at[0, pl.ds(0, GROUP - 1), :, pl.ds(0, part)], msend.at[0], mrecv.at[item]).wait_recv()

    def y_copy(i, u, d, k):
        at = species.at[me, peer(u, d), :, lanes(PARTS - SINGLE + k)]
        return remote(at, at, ysend.at[0], yrecv.at[chips - 1 - i, u, k], col, other_chip(i))

    def y_arrivals(u, k):
        for i in range(1, chips):
            total_of(species.at[0, pl.ds(0, GROUP), :, pl.ds(0, part)], ysend.at[0], yrecv.at[i - 1, u, k]).wait_recv()
            for d in range(GROUP):
                hand_on(other_chip(i), peer(u, d), PARTS - SINGLE + k)

    def group_item(u, r):
        item = u * per + r
        b = me if r < SINGLE else other_chip(r - SINGLE)
        q = PARTS - SINGLE + r if r < SINGLE else 1
        j = peer(u, 0)

        def start(t):
            push(lhs, sums_group[pick(t)], b, j, q * part_rows + t * 2)

        def done(t):
            one, two = sums_group[pick(t)]
            acc = pltpu.matmul_pop(one) + pltpu.matmul_pop(two)
            inv = 1.0 / acc[2 * span:2 * span + 8]
            for n in range(GROUP):
                value = acc[n * rows:(n + 1) * rows] + acc[span + n * rows:span + (n + 1) * rows]
                stage[item, n, :, at_block(t)] = value * inv[:rows]

        def sent():
            species[b, j, :, lanes(q)] = stage[item, member]
            for d in range(1, GROUP):
                member_copy(item, d, b, j, q).start()
            if r < SINGLE:
                for i in range(1, chips):
                    y_copy(i, u, 0, r).start()
            hand_on(b, j, q)

        return start, done, sent

    def single_arrivals(u, k):
        member_arrivals(u * per + k)
        for d in range(1, GROUP):
            for i in range(1, chips):
                y_copy(i, u, d, k).start()
            hand_on(me, peer(u, d), PARTS - SINGLE + k)

    def double_arrivals(u, i):
        member_arrivals(u * per + SINGLE + i)
        for d in range(1, GROUP):
            hand_on(other_chip(i), peer(u, d), 1)

    locals_each = GROUP * chips

    def local_item(u, k):
        b, j = other_chip(lax.rem(k, chips)), peer(u, k // chips)

        def start(t):
            push(lhs_own, sums_own[pick(t)], b, j, t * 2)

        def done(t):
            one, two = sums_own[pick(t)]
            acc = pltpu.matmul_pop(one) + pltpu.matmul_pop(two)
            inv = 1.0 / acc[2 * pad:2 * pad + 8]
            species[b, j, :, at_block(t)] = (acc[:rows] + acc[pad:pad + rows]) * inv[:rows]

        return start, done, lambda: hand_on(b, j, 0)

    @pl.loop(0, groups)
    def _(u):
        @pl.when(u > 0)
        def _():
            first_arrival(0, u).wait_recv()
            for d in range(1, GROUP):
                second_copy(u, 0, d).start()

        before = None
        for r in range(per):
            if r == 1:
                for i in range(1, chips):
                    first_arrival(i, u).wait_recv()
                    for d in range(1, GROUP):
                        second_copy(u, i, d).start()

                @pl.when(u == 0)
                def _():
                    total_of(curve.at[pl.ds(0, chips - 1), :, pl.ds(0, 2 * part_rows)], ksend.at[0], krecv.at[0]).wait_recv()

            start, done, sent = group_item(u, r)
            run(start, done, sent, before)
            before = functools.partial(close, done, sent)
        before()

        run(*local_item(u, 0))
        for d in range(GROUP):
            if d > 0:
                second_arrival(u, d).wait_recv()

            @pl.loop(max(1, d * chips), (d + 1) * chips)
            def _(k):
                _, done, sent = local_item(u, k - 1)
                run(*local_item(u, k), before=functools.partial(close, done, sent))

            @pl.when(u > 0)
            def _():
                if d < 2:
                    for i in range(d * chips // 2, (d + 1) * chips // 2):
                        double_arrivals(u - 1, i)
                if d % 2 == 1:
                    y_arrivals(u - 1, d // 2)

            if d > 1:
                single_arrivals(u, d - 2)

        _, done, sent = local_item(u, locals_each - 1)
        close(done, sent)

    for i in range(chips):
        at = lam_ref.at[other_chip(i)]
        remote(at, at, lsend.at[0], lrecv.at[0], col, partner).start()

    for i in range(chips):
        double_arrivals(last, i)
    for s in range(SINGLE):
        y_arrivals(last, s)

    total_of(tab.at[pl.ds(0, cols - 1)], tsend.at[0], trecv.at[0]).wait_send()
    total_of(curve.at[pl.ds(0, chips - 1), :, pl.ds(0, 2 * part_rows)], ksend.at[0], krecv.at[0]).wait_send()
    total_of(lam_ref.at[0, pl.ds(0, chips * groups - 1)], asend.at[0], lrecv.at[0]).wait_send()
    total_of(lam_ref.at[pl.ds(0, chips), pl.ds(0, (GROUP - 1) * groups)], bsend.at[0], lrecv.at[0]).wait_send()
    total_of(stage.at[:, pl.ds(0, GROUP - 1)], msend.at[0], precv.at[0]).wait_send()
    total_of(species.at[pl.ds(0, chips - 1), :, :, pl.ds(0, SINGLE * part)], ysend.at[0], precv.at[0]).wait_send()
    total_of(lam_ref.at[pl.ds(0, chips)], lsend.at[0], lrecv.at[0]).wait()
    total_of(species.at[pl.ds(0, chips)], psend.at[0], precv.at[0]).wait()


def scoped_kernel(cols, bins, total_pts, rows, pad, *refs):
    def pair(m):
        return tuple(pltpu.ACC(q)((m, 256), jnp.float32) for q in range(2))

    def body(sums):
        kernel(cols, bins, total_pts, rows, *refs, sums)

    shapes = tuple((pair(m), pair(m)) for m in (2 * GROUP * rows + 16, 2 * pad + 16))
    pl.run_scoped(body, shapes)


def write_kernel(species, lam, out_ref, lam_out, sem):
    bins, cols, _, width = species.shape
    for b in range(bins):
        for j in range(cols):
            pltpu.make_async_copy(species.at[b, j], out_ref.at[:, pl.ds((b * cols + j) * width, width)], sem.at[0]).start()
    keep = pltpu.make_async_copy(lam, lam_out, sem.at[1])
    keep.start()
    pltpu.make_async_copy(out_ref, out_ref, sem.at[0]).wait()
    keep.wait()


def per_device(slope, curvature, target_mean, target_var, table):
    cols = lax.axis_size("col")
    bins = lax.axis_size("bin")
    all_species, pts = table.shape
    rows = all_species // cols
    pad = -(-rows // 8) * 8
    total_pts = pts * cols
    per_shard = slope.shape[0]
    sub = per_shard // cols // LANES
    width = sub * LANES
    chips = bins // 2
    groups = cols // GROUP
    items = groups * (SINGLE + chips)
    side = max(1, min(GROUP, LANES // pts))
    packed = (groups, GROUP // side, rows, side * pts)

    def blocks(a):
        return a.reshape(cols, sub, LANES)

    placed = table.reshape(cols, rows, pts)
    vmem = pl.BlockSpec(memory_space=pltpu.VMEM)
    hbm = pl.BlockSpec(memory_space=pltpu.HBM)
    dma = pltpu.SemaphoreType.DMA
    one = dma((1,))
    species, lam = pl.pallas_call(
        functools.partial(scoped_kernel, cols, bins, total_pts, rows, pad),
        out_shape=(
            jax.ShapeDtypeStruct((bins, cols, rows, width), jnp.float32),
            jax.ShapeDtypeStruct((bins, cols, sub, LANES), jnp.float32),
        ),
        in_specs=[hbm] * 5,
        out_specs=(vmem, vmem),
        scratch_shapes=[
            pltpu.VMEM((3, sub, LANES), jnp.float32),
            pltpu.VMEM((bins, cols, sub, LANES), jnp.float32),
            pltpu.VMEM((cols, rows, pts), jnp.float32),
            pltpu.VMEM(packed, jnp.float32),
            pltpu.VMEM((cols, *packed[1:]), jnp.float32),
            pltpu.VMEM((2 * GROUP * rows + 16, total_pts), jnp.bfloat16),
            pltpu.VMEM((2 * pad + 16, total_pts), jnp.bfloat16),
            pltpu.VMEM((2, STRIDE, 2 * LANES), jnp.float32),
            pltpu.VMEM((items, GROUP, rows, width // PARTS), jnp.float32),
            dma((5,)), pltpu.SemaphoreType.REGULAR,
            one, one, one, one, one, dma((chips, groups)),
            one, dma((groups, GROUP)),
            one, one, one, dma((items,)),
            one, dma((chips - 1, groups, SINGLE)), one, one,
        ],
        compiler_params=pltpu.CompilerParams(collective_id=0, has_side_effects=True, vmem_limit_bytes=24 << 20),
    )(*[
        pltpu.with_memory_space_constraint(a, pltpu.HBM)
        for a in (blocks(slope), blocks(curvature), blocks(target_mean), blocks(target_var), placed)
    ])
    species_mean, lam = pl.pallas_call(
        write_kernel,
        out_shape=(
            jax.ShapeDtypeStruct((rows, per_shard * bins), jnp.float32),
            jax.ShapeDtypeStruct((bins, cols, sub, LANES), jnp.float32),
        ),
        in_specs=[vmem, vmem],
        out_specs=(hbm, hbm),
        scratch_shapes=[dma((2,))],
        compiler_params=pltpu.CompilerParams(vmem_limit_bytes=4 << 20),
    )(species, lam)
    return species_mean, lam.reshape(-1)


def solution(mesh):
    placed = (P("bin"), P("bin"), P("bin"), P("bin"), P(None, "col"))
    return jax.shard_map(
        per_device, mesh=mesh, in_specs=placed, out_specs=(P("col", None), P()), check_vma=False
    )
```

```python
import functools
import math
import jax
import jax.numpy as jnp
from jax import lax
from jax.experimental import pallas as pl
from jax.experimental.pallas import tpu as pltpu
from jax.sharding import PartitionSpec as P

ITERS = 3
LANES = 128
LOG2E = math.log2(math.e)
MESH = pl.DeviceIdType.MESH
UNROLL = 32
STRIDE = 32
DEPTH = 256
GROUP = 4
PARTS = 4
SINGLE = 2


def kernel(
    cols, bins, total_pts, rows,
    slope_hbm, curve_hbm, mean_hbm, var_hbm, placed_hbm,
    species, lam_ref,
    own, curve, placed, packed, tab, lhs, consts, stage,
    isem, far, tsend, trecv, ksend, krecv, asend, arecv, bsend, brecv,
    lsend, lrecv, msend, mrecv, ysend, yrecv, psend, precv,
    sums,
):
    col = lax.axis_index("col")
    me = lax.axis_index("bin")
    core = lax.rem(me, 2)
    partner = me + 1 - 2 * core
    chips = bins // 2
    groups = cols // GROUP
    member = lax.rem(col, GROUP)
    group = col // GROUP
    last = groups - 1
    sub = own.shape[1]
    width = sub * LANES
    part = width // PARTS
    part_rows = sub // PARTS
    pts = total_pts // cols
    side = packed.shape[3] // pts
    per = SINGLE + chips
    blocks = part_rows // 2
    lag = blocks % 2 == 0

    def other_chip(i):
        return lax.rem(me + 2 * i, bins)

    def peer(u, d):
        return lax.rem(group + u, groups) * GROUP + lax.rem(member + d, GROUP)

    def remote(src, dst, send, recv, c, b):
        return pltpu.make_async_remote_copy(
            src_ref=src, dst_ref=dst, send_sem=send, recv_sem=recv,
            device_id=(c, b), device_id_type=MESH,
        )

    def total_of(ref, send, recv):
        return remote(ref, ref, send, recv, col, partner)

    def greet(sem, c, b):
        pl.semaphore_signal(sem, inc=1, device_id=(c, b), device_id_type=MESH)

    barrier = pltpu.get_barrier_semaphore()
    greet(barrier, col, partner)
    for d in range(1, GROUP):
        greet(barrier, peer(0, d), me)
    for i in range(1, chips):
        greet(barrier, col, other_chip(i))

    def greet_group(sem, g):
        for d in range(GROUP):
            greet(sem, g * GROUP + d, me)
        for i in range(1, chips):
            greet(sem, g * GROUP + member, other_chip(i))

    @pl.loop(group + 1, groups)
    def _(g):
        greet_group(barrier, g)

    load_table = pltpu.make_async_copy(placed_hbm, placed, isem.at[4])
    load_table.start()
    loads = [
        pltpu.make_async_copy(a.at[col], own.at[n], isem.at[n])
        for n, a in enumerate((slope_hbm, mean_hbm, var_hbm))
    ]
    loads.append(pltpu.make_async_copy(curve_hbm, curve.at[me], isem.at[3]))
    for load in loads:
        load.start()

    for pair in sums:
        for acc in pair:
            pltpu.matmul_pop(acc)

    each = GROUP + chips - 1
    h = 1.0 / total_pts
    wide = STRIDE * h
    first = (lax.broadcasted_iota(jnp.int32, consts.shape[1:], 0).astype(jnp.float32) + 0.5) * h
    consts[0] = first
    consts[1] = wide * (2.0 * first + wide)

    load_table.wait()
    for g in range(groups):
        for p in range(GROUP // side):
            packed[g, p] = jnp.concatenate([placed[g * GROUP + p * side + n] for n in range(side)], axis=1)

    def table_copy(to):
        return remote(packed.at[to // GROUP], tab.at[col], tsend.at[0], trecv.at[0], to, me)

    def curve_copy(i):
        at = curve.at[me, :, pl.ds(0, 2 * part_rows)]
        return remote(at, at, ksend.at[0], krecv.at[0], col, other_chip(i))

    def enter():
        pl.semaphore_wait(barrier, (group + 1) * each)

        @pl.loop(0, group)
        def _(g):
            greet_group(far, g)

        @pl.loop(0, group)
        def _(g):
            for d in range(GROUP):
                table_copy(g * GROUP + d).start()

        for d in range(1, GROUP):
            table_copy(peer(0, d)).start()
        tab[col] = packed[group]

    for load in loads:
        load.wait()

    @pl.when(group == last)
    def _():
        enter()
        for i in range(1, chips):
            curve_copy(i).start()

    curve2 = curve[me, col] * LOG2E
    target = own[1]
    var = own[2]
    bend = jnp.exp2(curve2 * (2.0 * h * h))

    def newton(lam):
        lam2 = lam * LOG2E

        def begin(g):
            c = ((g * UNROLL).astype(jnp.float32) + 0.5) * h
            return jnp.exp2(c * (lam2 + curve2 * c)), jnp.exp2(h * (lam2 + curve2 * (2.0 * c + h)))

        def body(g, carry):
            total, mom, e, ratio = carry
            later = begin(g + 1)
            c = ((g * UNROLL).astype(jnp.float32) + 0.5) * h
            run = e
            runs = e
            for i in range(1, UNROLL):
                e = e * ratio
                if i < UNROLL - 1:
                    ratio = ratio * bend
                run = run + e
                runs = runs + run
            return total + run, mom + (c * run + h * (UNROLL * run - runs)), *later

        zero = jnp.zeros_like(lam)
        total, mom, _, _ = lax.fori_loop(0, total_pts // UNROLL, body, (zero, zero, *begin(jnp.int32(0))))
        return lam + (target - mom / total) / var

    lam_ref[me, col] = lax.fori_loop(0, ITERS, lambda _, lam: newton(lam), own[0])

    @pl.when(group < last)
    def _():
        enter()

    def first_copy(i, u):
        at = lam_ref.at[me, col]
        return remote(at, at, asend.at[0], arecv.at[(chips - i) % chips, lax.rem(groups - u, groups)], peer(u, 0), other_chip(i))

    def first_arrival(i, u):
        b, j = other_chip(i), peer(u, 0)
        at = lam_ref.at[b, j]
        return remote(at, at, asend.at[0], arecv.at[i, u], j, b)

    def second_copy(u, i, d):
        at = lam_ref.at[other_chip(i), peer(u, 0)]
        return remote(at, at, bsend.at[0], brecv.at[u, member], peer(0, d), me)

    def second_arrival(u, d):
        at = lam_ref.at[pl.ds(0, chips), 0]
        return remote(at, at, bsend.at[0], brecv.at[u, lax.rem(member + d, GROUP)], col, partner)

    for i in range(1, chips):
        first_copy(i, 0).start()
    for d in range(1, GROUP):
        second_copy(0, 0, d).start()

    @pl.when(group < last)
    def _():
        for i in range(1, chips):
            curve_copy(i).start()
        pl.semaphore_wait(far, (last - group) * each)

        @pl.loop(group + 1, groups)
        def _(g):
            for d in range(GROUP):
                table_copy(g * GROUP + d).start()

    @pl.loop(1, groups)
    def _(u):
        for i in range(chips):
            first_copy(i, u).start()

    total_of(tab.at[pl.ds(0, cols - 1)], tsend.at[0], trecv.at[0]).wait_recv()

    def split(full):
        high = full.astype(jnp.bfloat16).astype(jnp.float32)
        return jnp.concatenate([high, full - high, jnp.ones((16, total_pts), jnp.float32)], axis=0).astype(jnp.bfloat16)

    def gathered(n):
        return jnp.concatenate([tab[t, n // side][:, n % side * pts:(n % side + 1) * pts] for t in range(cols)], axis=1)

    span = GROUP * rows
    lhs[...] = split(jnp.concatenate([gathered(n) for n in range(GROUP)], axis=0))

    def lanes(q):
        return pl.ds(pl.multiple_of(q * part, LANES), part)

    def push(left, accs, b, j, r):
        lam_t = jnp.concatenate([lam_ref[b, j, pl.ds(r + n, 1)] for n in range(2)], axis=1) * LOG2E
        cur_t = jnp.concatenate([curve[b, j, pl.ds(r + n, 1)] for n in range(2)], axis=1) * LOG2E
        c = consts[0]
        e = jnp.exp2(c * (lam_t + cur_t * c))
        ratio = jnp.exp2(wide * lam_t + cur_t * consts[1])
        turn = jnp.broadcast_to(jnp.exp2(cur_t * (2.0 * wide * wide)), e.shape)
        steps = DEPTH // STRIDE
        tiles = total_pts // DEPTH
        for n in range(tiles):
            highs, lows = [], []
            for m in range(steps):
                e_hi = e.astype(jnp.bfloat16)
                highs.append(e_hi)
                lows.append((e - e_hi.astype(jnp.float32)).astype(jnp.bfloat16))
                if n < tiles - 1 or m < steps - 1:
                    e = e * ratio
                    ratio = ratio * turn
            for q, pieces in enumerate((highs, lows)):
                pltpu.matmul_push_rhs(jnp.concatenate(pieces, axis=0), n % 2, q)
            piece = left[:, n * DEPTH:(n + 1) * DEPTH]
            for acc in accs:
                pltpu.matmul_acc_lhs(acc, piece, load_staged_rhs=n % 2)

    def pick(t):
        return (blocks - t) % 2

    def at_block(t):
        return pl.ds(t * 2 * LANES, 2 * LANES)

    def hand_on(b, j, q):
        at = species.at[b, j, :, lanes(q)]
        remote(at, at, psend.at[0], precv.at[0], col, partner).start()

    def member_copy(item, d, b, j, q):
        to = lax.rem(member + d, GROUP)
        return remote(stage.at[item, to], species.at[b, j, :, lanes(q)], msend.at[0], mrecv.at[item], group * GROUP + to, me)

    def member_arrivals(item):
        total_of(species.at[0, pl.ds(0, GROUP - 1), :, pl.ds(0, part)], msend.at[0], mrecv.at[item]).wait_recv()

    def y_copy(i, u, d, k):
        at = species.at[me, peer(u, d), :, lanes(PARTS - SINGLE + k)]
        return remote(at, at, ysend.at[0], yrecv.at[chips - 1 - i, u, k], col, other_chip(i))

    def y_arrivals(u, k):
        for i in range(1, chips):
            total_of(species.at[0, pl.ds(0, GROUP), :, pl.ds(0, part)], ysend.at[0], yrecv.at[i - 1, u, k]).wait_recv()
            for d in range(GROUP):
                hand_on(other_chip(i), peer(u, d), PARTS - SINGLE + k)

    count = SINGLE + chips
    doubles_from = groups * count
    locals_from = doubles_from + groups * chips
    others = (GROUP - 1) * chips
    total = locals_from + groups * others
    spare = groups * per

    def place(n):
        u0, r0 = n // count, lax.rem(n, count)
        n1 = jnp.maximum(n - doubles_from, 0)
        u1, i1 = n1 // chips, lax.rem(n1, chips)
        n2 = jnp.maximum(n - locals_from, 0)
        u2, m2 = n2 // others, lax.rem(n2, others)
        single = jnp.logical_and(n < doubles_from, r0 < SINGLE)
        double = jnp.logical_and(n >= doubles_from, n < locals_from)
        late = n >= locals_from
        u = jnp.where(late, u2, jnp.where(double, u1, u0))
        i = jnp.where(late, lax.rem(m2, chips), jnp.where(double, i1, jnp.maximum(r0 - SINGLE, 0)))
        b = other_chip(i)
        j = peer(u, jnp.where(late, 1 + m2 // chips, 0))
        q = jnp.where(single, PARTS - SINGLE + r0, jnp.where(double, 1, 0))
        item = jnp.where(single, u * per + r0, jnp.where(double, u * per + SINGLE + i, spare))
        return single, u, r0, b, j, q, item

    def start(n, t):
        _, _, _, b, j, q, _ = place(n)
        push(lhs, sums[pick(t)], b, j, q * part_rows + t * 2)

    def done(n, t):
        item = place(n)[6]
        one, two = sums[pick(t)]
        acc = pltpu.matmul_pop(one) + pltpu.matmul_pop(two)
        inv = 1.0 / acc[2 * span:2 * span + 8]
        for g in range(GROUP):
            value = acc[g * rows:(g + 1) * rows] + acc[span + g * rows:span + (g + 1) * rows]
            stage[item, g, :, at_block(t)] = value * inv[:rows]

    def keep(n):
        _, _, _, b, j, q, item = place(n)
        species[b, j, :, lanes(q)] = stage[item, member]

    def sent(n):
        single, u, r, b, j, q, item = place(n)

        @pl.when(item < spare)
        def _():
            for d in range(1, GROUP):
                member_copy(item, d, b, j, q).start()

        @pl.when(single)
        def _():
            for i in range(1, chips):
                y_copy(i, u, 0, r).start()

        hand_on(b, j, q)

    def single_arrivals(u, k):
        member_arrivals(u * per + k)
        for d in range(1, GROUP):
            for i in range(1, chips):
                y_copy(i, u, d, k).start()
            hand_on(me, peer(u, d), PARTS - SINGLE + k)

    def double_arrivals(u, i):
        member_arrivals(u * per + SINGLE + i)
        for d in range(1, GROUP):
            hand_on(other_chip(i), peer(u, d), 1)

    def ready(n):
        @pl.when(n < doubles_from)
        def _():
            u, r = n // count, lax.rem(n, count)

            @pl.when(jnp.logical_and(r == 0, u > 0))
            def _():
                first_arrival(0, u).wait_recv()
                for d in range(1, GROUP):
                    second_copy(u, 0, d).start()

            @pl.when(r == SINGLE + 1)
            def _():
                for i in range(1, chips):
                    first_arrival(i, u).wait_recv()
                    for d in range(1, GROUP):
                        second_copy(u, i, d).start()

                @pl.when(u == 0)
                def _():
                    total_of(curve.at[pl.ds(0, chips - 1), :, pl.ds(0, 2 * part_rows)], ksend.at[0], krecv.at[0]).wait_recv()

        m = n - locals_from

        @pl.when(jnp.logical_and(m >= 0, lax.rem(m, chips) == 0))
        def _():
            second_arrival(m // others, 1 + lax.rem(m, others) // chips).wait_recv()

    events = (
        (doubles_from, 2, groups * SINGLE, lambda e: single_arrivals(e // SINGLE, lax.rem(e, SINGLE))),
        (locals_from + 4, 3, groups * SINGLE, lambda e: y_arrivals(e // SINGLE, lax.rem(e, SINGLE))),
        (locals_from + 5, 2, groups * chips, lambda e: double_arrivals(e // chips, lax.rem(e, chips))),
    )

    def served(n):
        for begin, every, number, event in events:
            m = n - begin

            @pl.when(jnp.logical_and(jnp.logical_and(m >= 0, m < number * every), lax.rem(m, every) == 0))
            def _():
                event(m // every)

    @pl.loop(0, total)
    def _(n):
        ready(n)
        back = jnp.maximum(n - 1, 0)
        for t in range(blocks):
            start(n, t)
            if t > 0:
                done(n, t - 1)
            elif lag:
                done(back, blocks - 1)
                keep(back)
        if lag:
            @pl.when(n > 0)
            def _():
                sent(back)
        else:
            done(n, blocks - 1)
            keep(n)
            sent(n)
        served(n)

    if lag:
        done(total - 1, blocks - 1)
        keep(total - 1)
        sent(total - 1)

    for i in range(chips):
        at = lam_ref.at[other_chip(i)]
        remote(at, at, lsend.at[0], lrecv.at[0], col, partner).start()

    for begin, every, number, event in reversed(events):
        @pl.loop(max(0, min(number, -((begin - total) // every))), number)
        def _(e):
            event(e)


    total_of(tab.at[pl.ds(0, cols - 1)], tsend.at[0], trecv.at[0]).wait_send()
    total_of(curve.at[pl.ds(0, chips - 1), :, pl.ds(0, 2 * part_rows)], ksend.at[0], krecv.at[0]).wait_send()
    total_of(lam_ref.at[0, pl.ds(0, chips * groups - 1)], asend.at[0], lrecv.at[0]).wait_send()
    total_of(lam_ref.at[pl.ds(0, chips), pl.ds(0, (GROUP - 1) * groups)], bsend.at[0], lrecv.at[0]).wait_send()
    total_of(stage.at[pl.ds(0, spare), pl.ds(0, GROUP - 1)], msend.at[0], precv.at[0]).wait_send()
    total_of(species.at[pl.ds(0, chips - 1), :, :, pl.ds(0, SINGLE * part)], ysend.at[0], precv.at[0]).wait_send()
    total_of(lam_ref.at[pl.ds(0, chips)], lsend.at[0], lrecv.at[0]).wait()
    total_of(species.at[pl.ds(0, chips)], psend.at[0], precv.at[0]).wait()


def scoped_kernel(cols, bins, total_pts, rows, *refs):
    def pair(m):
        return tuple(pltpu.ACC(q)((m, 256), jnp.float32) for q in range(2))

    def body(sums):
        kernel(cols, bins, total_pts, rows, *refs, sums)

    m = 2 * GROUP * rows + 16
    pl.run_scoped(body, (pair(m), pair(m)))


def write_kernel(species, lam, out_ref, lam_out, sem):
    bins, cols, _, width = species.shape
    for b in range(bins):
        for j in range(cols):
            pltpu.make_async_copy(species.at[b, j], out_ref.at[:, pl.ds((b * cols + j) * width, width)], sem.at[0]).start()
    keep = pltpu.make_async_copy(lam, lam_out, sem.at[1])
    keep.start()
    pltpu.make_async_copy(out_ref, out_ref, sem.at[0]).wait()
    keep.wait()


def per_device(slope, curvature, target_mean, target_var, table):
    cols = lax.axis_size("col")
    bins = lax.axis_size("bin")
    all_species, pts = table.shape
    rows = all_species // cols
    total_pts = pts * cols
    per_shard = slope.shape[0]
    sub = per_shard // cols // LANES
    width = sub * LANES
    chips = bins // 2
    groups = cols // GROUP
    items = groups * (SINGLE + chips)
    side = max(1, min(GROUP, LANES // pts))
    packed = (groups, GROUP // side, rows, side * pts)

    def blocks(a):
        return a.reshape(cols, sub, LANES)

    placed = table.reshape(cols, rows, pts)
    vmem = pl.BlockSpec(memory_space=pltpu.VMEM)
    hbm = pl.BlockSpec(memory_space=pltpu.HBM)
    dma = pltpu.SemaphoreType.DMA
    one = dma((1,))
    species, lam = pl.pallas_call(
        functools.partial(scoped_kernel, cols, bins, total_pts, rows),
        out_shape=(
            jax.ShapeDtypeStruct((bins, cols, rows, width), jnp.float32),
            jax.ShapeDtypeStruct((bins, cols, sub, LANES), jnp.float32),
        ),
        in_specs=[hbm] * 5,
        out_specs=(vmem, vmem),
        scratch_shapes=[
            pltpu.VMEM((3, sub, LANES), jnp.float32),
            pltpu.VMEM((bins, cols, sub, LANES), jnp.float32),
            pltpu.VMEM((cols, rows, pts), jnp.float32),
            pltpu.VMEM(packed, jnp.float32),
            pltpu.VMEM((cols, *packed[1:]), jnp.float32),
            pltpu.VMEM((2 * GROUP * rows + 16, total_pts), jnp.bfloat16),
            pltpu.VMEM((2, STRIDE, 2 * LANES), jnp.float32),
            pltpu.VMEM((items + 1, GROUP, rows, width // PARTS), jnp.float32),
            dma((5,)), pltpu.SemaphoreType.REGULAR,
            one, one, one, one, one, dma((chips, groups)),
            one, dma((groups, GROUP)),
            one, one, one, dma((items,)),
            one, dma((chips - 1, groups, SINGLE)), one, one,
        ],
        compiler_params=pltpu.CompilerParams(collective_id=0, has_side_effects=True, vmem_limit_bytes=24 << 20),
    )(*[
        pltpu.with_memory_space_constraint(a, pltpu.HBM)
        for a in (blocks(slope), blocks(curvature), blocks(target_mean), blocks(target_var), placed)
    ])
    species_mean, lam = pl.pallas_call(
        write_kernel,
        out_shape=(
            jax.ShapeDtypeStruct((rows, per_shard * bins), jnp.float32),
            jax.ShapeDtypeStruct((bins, cols, sub, LANES), jnp.float32),
        ),
        in_specs=[vmem, vmem],
        out_specs=(hbm, hbm),
        scratch_shapes=[dma((2,))],
        compiler_params=pltpu.CompilerParams(vmem_limit_bytes=4 << 20),
    )(species, lam)
    return species_mean, lam.reshape(-1)


def solution(mesh):
    placed = (P("bin"), P("bin"), P("bin"), P("bin"), P(None, "col"))
    return jax.shard_map(
        per_device, mesh=mesh, in_specs=placed, out_specs=(P("col", None), P()), check_vma=False
    )
```

```python
import functools
import math
import jax
import jax.numpy as jnp
from jax import lax
from jax.experimental import pallas as pl
from jax.experimental.pallas import tpu as pltpu
from jax.sharding import PartitionSpec as P

ITERS = 3
LANES = 128
LOG2E = math.log2(math.e)
MESH = pl.DeviceIdType.MESH
UNROLL = 32
STRIDE = 32
DEPTH = 256
GROUP = 4
RANK = 2
PARTS = 4
SINGLE = 2


def kernel(
    cols, bins, total_pts, rows,
    slope_hbm, curve_hbm, mean_hbm, var_hbm, placed_hbm,
    species, lam_ref,
    own, curve, placed, packed, tab, lhs, consts, stage,
    isem, far, tsend, trecv, ksend, krecv, asend, arecv, bsend, brecv,
    lsend, lrecv, msend, mrecv, ysend, yrecv, psend, precv,
    sums,
):
    col = lax.axis_index("col")
    me = lax.axis_index("bin")
    core = lax.rem(me, 2)
    partner = me + 1 - 2 * core
    chips = bins // 2
    groups = cols // GROUP
    member = lax.rem(col, GROUP)
    group = col // GROUP
    last = groups - 1
    sub = own.shape[1]
    width = sub * LANES
    part = width // PARTS
    part_rows = sub // PARTS
    pts = total_pts // cols
    side = packed.shape[3] // pts
    per = SINGLE + chips
    blocks = part_rows // 2
    lag = blocks % 2 == 0

    def other_chip(i):
        return lax.rem(me + 2 * i, bins)

    def peer(u, d):
        return lax.rem(group + u, groups) * GROUP + lax.rem(member + d, GROUP)

    def remote(src, dst, send, recv, c, b):
        return pltpu.make_async_remote_copy(
            src_ref=src, dst_ref=dst, send_sem=send, recv_sem=recv,
            device_id=(c, b), device_id_type=MESH,
        )

    def total_of(ref, send, recv):
        return remote(ref, ref, send, recv, col, partner)

    def greet(sem, c, b):
        pl.semaphore_signal(sem, inc=1, device_id=(c, b), device_id_type=MESH)

    barrier = pltpu.get_barrier_semaphore()
    rank = col // RANK
    ranks = cols // RANK

    def greet_rank(sem, k):
        for d in range(RANK):
            greet(sem, k * RANK + d, me)

    def greet_chips(sem, g):
        for i in range(1, chips):
            greet(sem, g * GROUP + member, other_chip(i))

    greet(barrier, col, partner)
    for d in range(1, RANK):
        greet(barrier, rank * RANK + lax.rem(col + d, RANK), me)

    @pl.loop(group, groups)
    def _(g):
        greet_chips(barrier, g)

    @pl.loop(rank + 1, ranks)
    def _(k):
        greet_rank(barrier, k)

    load_table = pltpu.make_async_copy(placed_hbm, placed, isem.at[4])
    load_table.start()
    loads = [
        pltpu.make_async_copy(a.at[col], own.at[n], isem.at[n])
        for n, a in enumerate((slope_hbm, mean_hbm, var_hbm))
    ]
    loads.append(pltpu.make_async_copy(curve_hbm, curve.at[me], isem.at[3]))
    for load in loads:
        load.start()

    for pair in sums:
        for acc in pair:
            pltpu.matmul_pop(acc)

    h = 1.0 / total_pts
    wide = STRIDE * h
    first = (lax.broadcasted_iota(jnp.int32, consts.shape[1:], 0).astype(jnp.float32) + 0.5) * h
    consts[0] = first
    consts[1] = wide * (2.0 * first + wide)

    load_table.wait()
    for g in range(groups):
        for p in range(GROUP // side):
            packed[g, p] = jnp.concatenate([placed[g * GROUP + p * side + n] for n in range(side)], axis=1)

    def table_copy(to):
        return remote(packed.at[to // GROUP], tab.at[col], tsend.at[0], trecv.at[0], to, me)

    def curve_copy(i):
        at = curve.at[me, :, pl.ds(0, 2 * part_rows)]
        return remote(at, at, ksend.at[0], krecv.at[0], col, other_chip(i))

    def enter():
        pl.semaphore_wait(barrier, (rank + 1) * RANK + (group + 1) * (chips - 1))

        @pl.loop(0, rank)
        def _(k):
            greet_rank(far, k)

        @pl.loop(0, group)
        def _(g):
            greet_chips(far, g)

        @pl.loop(0, rank)
        def _(k):
            for d in range(RANK):
                table_copy(k * RANK + d).start()

        for d in range(1, RANK):
            table_copy(rank * RANK + lax.rem(col + d, RANK)).start()
        tab[col] = packed[group]
        for i in range(1, chips):
            curve_copy(i).start()

    for load in loads:
        load.wait()

    @pl.when(rank > 0)
    def _():
        enter()

    curve2 = curve[me, col] * LOG2E
    target = own[1]
    var = own[2]
    bend = jnp.exp2(curve2 * (2.0 * h * h))

    def newton(lam):
        lam2 = lam * LOG2E

        def begin(g):
            c = ((g * UNROLL).astype(jnp.float32) + 0.5) * h
            return jnp.exp2(c * (lam2 + curve2 * c)), jnp.exp2(h * (lam2 + curve2 * (2.0 * c + h)))

        def body(g, carry):
            total, mom, e, ratio = carry
            later = begin(g + 1)
            c = ((g * UNROLL).astype(jnp.float32) + 0.5) * h
            run = e
            runs = e
            for i in range(1, UNROLL):
                e = e * ratio
                if i < UNROLL - 1:
                    ratio = ratio * bend
                run = run + e
                runs = runs + run
            return total + run, mom + (c * run + h * (UNROLL * run - runs)), *later

        zero = jnp.zeros_like(lam)
        total, mom, _, _ = lax.fori_loop(0, total_pts // UNROLL, body, (zero, zero, *begin(jnp.int32(0))))
        return lam + (target - mom / total) / var

    lam_ref[me, col] = lax.fori_loop(0, ITERS, lambda _, lam: newton(lam), own[0])

    @pl.when(rank == 0)
    def _():
        enter()

    def first_copy(i, u):
        at = lam_ref.at[me, col]
        return remote(at, at, asend.at[0], arecv.at[(chips - i) % chips, lax.rem(groups - u, groups)], peer(u, 0), other_chip(i))

    def first_arrival(i, u):
        b, j = other_chip(i), peer(u, 0)
        at = lam_ref.at[b, j]
        return remote(at, at, asend.at[0], arecv.at[i, u], j, b)

    def second_copy(u, i, d):
        at = lam_ref.at[other_chip(i), peer(u, 0)]
        return remote(at, at, bsend.at[0], brecv.at[u, member], peer(0, d), me)

    def second_arrival(u, d):
        at = lam_ref.at[pl.ds(0, chips), 0]
        return remote(at, at, bsend.at[0], brecv.at[u, lax.rem(member + d, GROUP)], col, partner)

    for i in range(1, chips):
        first_copy(i, 0).start()
    @pl.when(rank < ranks - 1)
    def _():
        pl.semaphore_wait(far, (ranks - 1 - rank) * RANK + (last - group) * (chips - 1))

        @pl.loop(rank + 1, ranks)
        def _(k):
            for d in range(RANK):
                table_copy(k * RANK + d).start()

    for d in range(1, GROUP):
        second_copy(0, 0, d).start()

    @pl.loop(1, groups)
    def _(u):
        for i in range(chips):
            first_copy(i, u).start()

    total_of(tab.at[pl.ds(0, cols - 1)], tsend.at[0], trecv.at[0]).wait_recv()

    def split(full):
        high = full.astype(jnp.bfloat16).astype(jnp.float32)
        return jnp.concatenate([high, full - high, jnp.ones((16, total_pts), jnp.float32)], axis=0).astype(jnp.bfloat16)

    def gathered(n):
        return jnp.concatenate([tab[t, n // side][:, n % side * pts:(n % side + 1) * pts] for t in range(cols)], axis=1)

    span = GROUP * rows
    lhs[...] = split(jnp.concatenate([gathered(n) for n in range(GROUP)], axis=0))

    def lanes(q):
        return pl.ds(pl.multiple_of(q * part, LANES), part)

    def push(left, accs, b, j, r):
        lam_t = jnp.concatenate([lam_ref[b, j, pl.ds(r + n, 1)] for n in range(2)], axis=1) * LOG2E
        cur_t = jnp.concatenate([curve[b, j, pl.ds(r + n, 1)] for n in range(2)], axis=1) * LOG2E
        c = consts[0]
        e = jnp.exp2(c * (lam_t + cur_t * c))
        ratio = jnp.exp2(wide * lam_t + cur_t * consts[1])
        turn = jnp.broadcast_to(jnp.exp2(cur_t * (2.0 * wide * wide)), e.shape)
        steps = DEPTH // STRIDE
        tiles = total_pts // DEPTH
        for n in range(tiles):
            highs, lows = [], []
            for m in range(steps):
                e_hi = e.astype(jnp.bfloat16)
                highs.append(e_hi)
                lows.append(e - e_hi.astype(jnp.float32))
                if n < tiles - 1 or m < steps - 1:
                    e = e * ratio
                    ratio = ratio * turn
            for q, pieces in enumerate((highs, lows)):
                pltpu.matmul_push_rhs(jnp.concatenate(pieces, axis=0), n % 2, q)
            piece = left[:, n * DEPTH:(n + 1) * DEPTH]
            for acc in accs:
                pltpu.matmul_acc_lhs(acc, piece, load_staged_rhs=n % 2)

    def pick(t):
        return (blocks - t) % 2

    def at_block(t):
        return pl.ds(t * 2 * LANES, 2 * LANES)

    def hand_on(b, j, q):
        at = species.at[b, j, :, lanes(q)]
        remote(at, at, psend.at[0], precv.at[0], col, partner).start()

    def member_copy(item, d, b, j, q):
        to = lax.rem(member + d, GROUP)
        return remote(stage.at[item, to], species.at[b, j, :, lanes(q)], msend.at[0], mrecv.at[item], group * GROUP + to, me)

    def member_arrivals(item):
        total_of(species.at[0, pl.ds(0, GROUP - 1), :, pl.ds(0, part)], msend.at[0], mrecv.at[item]).wait_recv()

    def y_copy(i, u, d, k):
        at = species.at[me, peer(u, d), :, lanes(PARTS - SINGLE + k)]
        return remote(at, at, ysend.at[0], yrecv.at[chips - 1 - i, u, k], col, other_chip(i))

    def y_arrivals(u, k):
        for i in range(1, chips):
            total_of(species.at[0, pl.ds(0, GROUP), :, pl.ds(0, part)], ysend.at[0], yrecv.at[i - 1, u, k]).wait_recv()

            @pl.loop(0, GROUP)
            def _(d):
                hand_on(other_chip(i), peer(u, d), PARTS - SINGLE + k)

    count = SINGLE + chips
    doubles_from = groups * count
    locals_from = doubles_from + groups * chips
    others = (GROUP - 1) * chips
    total = locals_from + groups * others
    spare = groups * per

    def place(n):
        u0, r0 = n // count, lax.rem(n, count)
        n1 = jnp.maximum(n - doubles_from, 0)
        u1, i1 = n1 // chips, lax.rem(n1, chips)
        n2 = jnp.maximum(n - locals_from, 0)
        u2, m2 = n2 // others, lax.rem(n2, others)
        single = jnp.logical_and(n < doubles_from, r0 < SINGLE)
        double = jnp.logical_and(n >= doubles_from, n < locals_from)
        late = n >= locals_from
        u = jnp.where(late, u2, jnp.where(double, u1, u0))
        i = jnp.where(late, lax.rem(m2, chips), jnp.where(double, i1, jnp.maximum(r0 - SINGLE, 0)))
        b = other_chip(i)
        j = peer(u, jnp.where(late, 1 + m2 // chips, 0))
        q = jnp.where(single, PARTS - SINGLE + r0, jnp.where(double, 1, 0))
        item = jnp.where(single, u * per + r0, jnp.where(double, u * per + SINGLE + i, spare))
        return single, u, r0, b, j, q, item

    def start(n, t):
        _, _, _, b, j, q, _ = place(n)
        push(lhs, sums[pick(t)], b, j, q * part_rows + t * 2)

    def done(n, t):
        item = place(n)[6]
        one, two = sums[pick(t)]
        acc = pltpu.matmul_pop(one) + pltpu.matmul_pop(two)
        inv = 1.0 / acc[2 * span:2 * span + 8]
        for g in range(GROUP):
            value = acc[g * rows:(g + 1) * rows] + acc[span + g * rows:span + (g + 1) * rows]
            stage[item, g, :, at_block(t)] = value * inv[:rows]

    def keep(n):
        _, _, _, b, j, q, item = place(n)
        species[b, j, :, lanes(q)] = stage[item, member]

    def sent(n):
        single, u, r, b, j, q, item = place(n)

        @pl.when(item < spare)
        def _():
            @pl.loop(1, GROUP)
            def _(d):
                member_copy(item, d, b, j, q).start()

        @pl.when(single)
        def _():
            for i in range(1, chips):
                y_copy(i, u, 0, r).start()

        hand_on(b, j, q)

    def single_arrivals(u, k):
        member_arrivals(u * per + k)

        @pl.loop(1, GROUP)
        def _(d):
            for i in range(1, chips):
                y_copy(i, u, d, k).start()
            hand_on(me, peer(u, d), PARTS - SINGLE + k)

    def double_arrivals(u, i):
        member_arrivals(u * per + SINGLE + i)

        @pl.loop(1, GROUP)
        def _(d):
            hand_on(other_chip(i), peer(u, d), 1)

    def ready(n):
        @pl.when(n < doubles_from)
        def _():
            u, r = n // count, lax.rem(n, count)

            @pl.when(jnp.logical_and(r == 0, u > 0))
            def _():
                first_arrival(0, u).wait_recv()
                for d in range(1, GROUP):
                    second_copy(u, 0, d).start()

            @pl.when(r == SINGLE + 1)
            def _():
                for i in range(1, chips):
                    first_arrival(i, u).wait_recv()
                    for d in range(1, GROUP):
                        second_copy(u, i, d).start()

                @pl.when(u == 0)
                def _():
                    total_of(curve.at[pl.ds(0, chips - 1), :, pl.ds(0, 2 * part_rows)], ksend.at[0], krecv.at[0]).wait_recv()

        m = n - locals_from

        @pl.when(jnp.logical_and(m >= 0, lax.rem(m, chips) == 0))
        def _():
            second_arrival(m // others, 1 + lax.rem(m, others) // chips).wait_recv()

    events = (
        (doubles_from, 2, groups * SINGLE, lambda e: single_arrivals(e // SINGLE, lax.rem(e, SINGLE))),
        (locals_from + 4, 3, groups * SINGLE, lambda e: y_arrivals(e // SINGLE, lax.rem(e, SINGLE))),
        (locals_from + 5, 2, groups * chips, lambda e: double_arrivals(e // chips, lax.rem(e, chips))),
    )

    def served(n):
        for begin, every, number, event in events:
            m = n - begin

            @pl.when(jnp.logical_and(jnp.logical_and(m >= 0, m < number * every), lax.rem(m, every) == 0))
            def _():
                event(m // every)

    @pl.loop(0, total)
    def _(n):
        ready(n)
        back = jnp.maximum(n - 1, 0)
        for t in range(blocks):
            start(n, t)
            if t > 0:
                done(n, t - 1)
            elif lag:
                done(back, blocks - 1)
                keep(back)
        if lag:
            @pl.when(n > 0)
            def _():
                sent(back)
        else:
            done(n, blocks - 1)
            keep(n)
            sent(n)
        served(n)

    if lag:
        done(total - 1, blocks - 1)
        keep(total - 1)
        sent(total - 1)

    for i in range(chips):
        at = lam_ref.at[other_chip(i)]
        remote(at, at, lsend.at[0], lrecv.at[0], col, partner).start()

    for begin, every, number, event in reversed(events):
        @pl.loop(max(0, min(number, -((begin - total) // every))), number)
        def _(e):
            event(e)


    total_of(tab.at[pl.ds(0, cols - 1)], tsend.at[0], trecv.at[0]).wait_send()
    total_of(curve.at[pl.ds(0, chips - 1), :, pl.ds(0, 2 * part_rows)], ksend.at[0], krecv.at[0]).wait_send()
    total_of(lam_ref.at[0, pl.ds(0, chips * groups - 1)], asend.at[0], lrecv.at[0]).wait_send()
    total_of(lam_ref.at[pl.ds(0, chips), pl.ds(0, (GROUP - 1) * groups)], bsend.at[0], lrecv.at[0]).wait_send()
    total_of(stage.at[pl.ds(0, spare), pl.ds(0, GROUP - 1)], msend.at[0], precv.at[0]).wait_send()
    total_of(species.at[pl.ds(0, chips - 1), :, :, pl.ds(0, SINGLE * part)], ysend.at[0], precv.at[0]).wait_send()
    total_of(lam_ref.at[pl.ds(0, chips)], lsend.at[0], lrecv.at[0]).wait()
    total_of(species.at[pl.ds(0, chips)], psend.at[0], precv.at[0]).wait()


def scoped_kernel(cols, bins, total_pts, rows, *refs):
    def pair(m):
        return tuple(pltpu.ACC(q)((m, 256), jnp.float32) for q in range(2))

    def body(sums):
        kernel(cols, bins, total_pts, rows, *refs, sums)

    m = 2 * GROUP * rows + 16
    pl.run_scoped(body, (pair(m), pair(m)))


def write_kernel(species, lam, out_ref, lam_out, sem):
    bins, cols, _, width = species.shape
    @pl.loop(0, bins)
    def _(b):
        for j in range(cols):
            to = pl.ds(pl.multiple_of((b * cols + j) * width, LANES), width)
            pltpu.make_async_copy(species.at[b, j], out_ref.at[:, to], sem.at[0]).start()

    keep = pltpu.make_async_copy(lam, lam_out, sem.at[1])
    keep.start()
    pltpu.make_async_copy(out_ref, out_ref, sem.at[0]).wait()
    keep.wait()


def per_device(slope, curvature, target_mean, target_var, table):
    cols = lax.axis_size("col")
    bins = lax.axis_size("bin")
    all_species, pts = table.shape
    rows = all_species // cols
    total_pts = pts * cols
    per_shard = slope.shape[0]
    sub = per_shard // cols // LANES
    width = sub * LANES
    chips = bins // 2
    groups = cols // GROUP
    items = groups * (SINGLE + chips)
    side = max(1, min(GROUP, LANES // pts))
    packed = (groups, GROUP // side, rows, side * pts)

    def blocks(a):
        return a.reshape(cols, sub, LANES)

    placed = table.reshape(cols, rows, pts)
    vmem = pl.BlockSpec(memory_space=pltpu.VMEM)
    hbm = pl.BlockSpec(memory_space=pltpu.HBM)
    dma = pltpu.SemaphoreType.DMA
    one = dma((1,))
    species, lam = pl.pallas_call(
        functools.partial(scoped_kernel, cols, bins, total_pts, rows),
        out_shape=(
            jax.ShapeDtypeStruct((bins, cols, rows, width), jnp.float32),
            jax.ShapeDtypeStruct((bins, cols, sub, LANES), jnp.float32),
        ),
        in_specs=[hbm] * 5,
        out_specs=(vmem, vmem),
        scratch_shapes=[
            pltpu.VMEM((3, sub, LANES), jnp.float32),
            pltpu.VMEM((bins, cols, sub, LANES), jnp.float32),
            pltpu.VMEM((cols, rows, pts), jnp.float32),
            pltpu.VMEM(packed, jnp.float32),
            pltpu.VMEM((cols, *packed[1:]), jnp.float32),
            pltpu.VMEM((2 * GROUP * rows + 16, total_pts), jnp.bfloat16),
            pltpu.VMEM((2, STRIDE, 2 * LANES), jnp.float32),
            pltpu.VMEM((items + 1, GROUP, rows, width // PARTS), jnp.float32),
            dma((5,)), pltpu.SemaphoreType.REGULAR,
            one, one, one, one, one, dma((chips, groups)),
            one, dma((groups, GROUP)),
            one, one, one, dma((items,)),
            one, dma((chips - 1, groups, SINGLE)), one, one,
        ],
        compiler_params=pltpu.CompilerParams(collective_id=0, has_side_effects=True, vmem_limit_bytes=24 << 20),
    )(*[
        pltpu.with_memory_space_constraint(a, pltpu.HBM)
        for a in (blocks(slope), blocks(curvature), blocks(target_mean), blocks(target_var), placed)
    ])
    species_mean, lam = pl.pallas_call(
        write_kernel,
        out_shape=(
            jax.ShapeDtypeStruct((rows, per_shard * bins), jnp.float32),
            jax.ShapeDtypeStruct((bins, cols, sub, LANES), jnp.float32),
        ),
        in_specs=[vmem, vmem],
        out_specs=(hbm, hbm),
        scratch_shapes=[dma((2,))],
        compiler_params=pltpu.CompilerParams(vmem_limit_bytes=4 << 20),
    )(species, lam)
    return species_mean, lam.reshape(-1)


def solution(mesh):
    placed = (P("bin"), P("bin"), P("bin"), P("bin"), P(None, "col"))
    return jax.shard_map(
        per_device, mesh=mesh, in_specs=placed, out_specs=(P("col", None), P()), check_vma=False
    )
```

```python
import functools
import math
import jax
import jax.numpy as jnp
from jax import lax
from jax.experimental import pallas as pl
from jax.experimental.pallas import tpu as pltpu
from jax.sharding import PartitionSpec as P

ITERS = 3
LANES = 128
LOG2E = math.log2(math.e)
MESH = pl.DeviceIdType.MESH
UNROLL = 32
STRIDE = 32
DEPTH = 256
GROUP = 4
RANK = 2
PARTS = 4
SINGLE = 2


def kernel(
    cols, bins, total_pts, rows,
    slope_hbm, curve_hbm, mean_hbm, var_hbm, placed_hbm,
    species, lam_ref,
    own, curve, placed, packed, tab, lhs, consts, stage,
    isem, far, tsend, trecv, ksend, krecv, asend, arecv, bsend, brecv,
    lsend, lrecv, msend, mrecv, ysend, yrecv, psend, precv,
    sums,
):
    col = lax.axis_index("col")
    me = lax.axis_index("bin")
    core = lax.rem(me, 2)
    partner = me + 1 - 2 * core
    chips = bins // 2
    groups = cols // GROUP
    member = lax.rem(col, GROUP)
    group = col // GROUP
    last = groups - 1
    sub = own.shape[1]
    width = sub * LANES
    part = width // PARTS
    part_rows = sub // PARTS
    pts = total_pts // cols
    side = packed.shape[3] // pts
    per = SINGLE + chips
    blocks = part_rows // 2
    lag = blocks % 2 == 0

    def other_chip(i):
        return lax.rem(me + 2 * i, bins)

    def peer(u, d):
        return lax.rem(group + u, groups) * GROUP + lax.rem(member + d, GROUP)

    def remote(src, dst, send, recv, c, b):
        return pltpu.make_async_remote_copy(
            src_ref=src, dst_ref=dst, send_sem=send, recv_sem=recv,
            device_id=(c, b), device_id_type=MESH,
        )

    def total_of(ref, send, recv):
        return remote(ref, ref, send, recv, col, partner)

    def greet(sem, c, b):
        pl.semaphore_signal(sem, inc=1, device_id=(c, b), device_id_type=MESH)

    barrier = pltpu.get_barrier_semaphore()
    rank = col // RANK
    ranks = cols // RANK

    def greet_rank(sem, k):
        for d in range(RANK):
            greet(sem, k * RANK + d, me)

    def greet_chips(sem, g):
        for i in range(1, chips):
            greet(sem, g * GROUP + member, other_chip(i))

    greet(barrier, col, partner)
    for d in range(1, RANK):
        greet(barrier, rank * RANK + lax.rem(col + d, RANK), me)

    @pl.loop(group, groups)
    def _(g):
        greet_chips(barrier, g)

    @pl.loop(rank + 1, ranks)
    def _(k):
        greet_rank(barrier, k)

    load_table = pltpu.make_async_copy(placed_hbm, placed, isem.at[4])
    load_table.start()
    loads = [
        pltpu.make_async_copy(a.at[col], own.at[n], isem.at[n])
        for n, a in enumerate((slope_hbm, mean_hbm, var_hbm))
    ]
    loads.append(pltpu.make_async_copy(curve_hbm, curve.at[me], isem.at[3]))
    for load in loads:
        load.start()

    for pair in sums:
        for acc in pair:
            pltpu.matmul_pop(acc)

    h = 1.0 / total_pts
    wide = STRIDE * h
    first = (lax.broadcasted_iota(jnp.int32, consts.shape[1:], 0).astype(jnp.float32) + 0.5) * h
    consts[0] = first
    consts[1] = wide * (2.0 * first + wide)

    load_table.wait()
    for g in range(groups):
        for p in range(GROUP // side):
            packed[g, p] = jnp.concatenate([placed[g * GROUP + p * side + n] for n in range(side)], axis=1)

    def table_copy(to):
        return remote(packed.at[to // GROUP], tab.at[col], tsend.at[0], trecv.at[0], to, me)

    def curve_copy(i):
        at = curve.at[me, :, pl.ds(0, 2 * part_rows)]
        return remote(at, at, ksend.at[0], krecv.at[0], col, other_chip(i))

    def enter():
        pl.semaphore_wait(barrier, (rank + 1) * RANK + (group + 1) * (chips - 1))

        @pl.loop(0, rank)
        def _(k):
            greet_rank(far, k)

        @pl.loop(0, group)
        def _(g):
            greet_chips(far, g)

        @pl.loop(0, rank)
        def _(k):
            for d in range(RANK):
                table_copy(k * RANK + d).start()

        for d in range(1, RANK):
            table_copy(rank * RANK + lax.rem(col + d, RANK)).start()
        tab[col] = packed[group]
        for i in range(1, chips):
            curve_copy(i).start()

    for load in loads:
        load.wait()

    @pl.when(rank > 0)
    def _():
        enter()

    curve2 = curve[me, col] * LOG2E
    target = own[1]
    var = own[2]
    bend = jnp.exp2(curve2 * (2.0 * h * h))

    def newton(lam):
        lam2 = lam * LOG2E

        def begin(g):
            c = ((g * UNROLL).astype(jnp.float32) + 0.5) * h
            return jnp.exp2(c * (lam2 + curve2 * c)), jnp.exp2(h * (lam2 + curve2 * (2.0 * c + h)))

        def body(g, carry):
            total, mom, e, ratio = carry
            later = begin(g + 1)
            c = ((g * UNROLL).astype(jnp.float32) + 0.5) * h
            run = e
            runs = e
            for i in range(1, UNROLL):
                e = e * ratio
                if i < UNROLL - 1:
                    ratio = ratio * bend
                run = run + e
                runs = runs + run
            return total + run, mom + (c * run + h * (UNROLL * run - runs)), *later

        zero = jnp.zeros_like(lam)
        total, mom, _, _ = lax.fori_loop(0, total_pts // UNROLL, body, (zero, zero, *begin(jnp.int32(0))))
        return lam + (target - mom / total) / var

    lam_ref[me, col] = lax.fori_loop(0, ITERS, lambda _, lam: newton(lam), own[0])

    @pl.when(rank == 0)
    def _():
        enter()

    def first_copy(i, u):
        at = lam_ref.at[me, col]
        return remote(at, at, asend.at[0], arecv.at[(chips - i) % chips, lax.rem(groups - u, groups)], peer(u, 0), other_chip(i))

    def first_arrival(i, u):
        b, j = other_chip(i), peer(u, 0)
        at = lam_ref.at[b, j]
        return remote(at, at, asend.at[0], arecv.at[i, u], j, b)

    def second_copy(u, i, d):
        at = lam_ref.at[other_chip(i), peer(u, 0)]
        return remote(at, at, bsend.at[0], brecv.at[u, member], peer(0, d), me)

    def second_arrival(u, d):
        at = lam_ref.at[pl.ds(0, chips), 0]
        return remote(at, at, bsend.at[0], brecv.at[u, lax.rem(member + d, GROUP)], col, partner)

    for i in range(1, chips):
        first_copy(i, 0).start()
    @pl.when(rank < ranks - 1)
    def _():
        pl.semaphore_wait(far, (ranks - 1 - rank) * RANK + (last - group) * (chips - 1))

        @pl.loop(rank + 1, ranks)
        def _(k):
            for d in range(RANK):
                table_copy(k * RANK + d).start()

    for d in range(1, GROUP):
        second_copy(0, 0, d).start()

    @pl.loop(1, groups)
    def _(u):
        for i in range(chips):
            first_copy(i, u).start()

    total_of(tab.at[pl.ds(0, cols - 1)], tsend.at[0], trecv.at[0]).wait_recv()

    def split(full):
        high = full.astype(jnp.bfloat16).astype(jnp.float32)
        return jnp.concatenate([high, full - high, jnp.ones((16, total_pts), jnp.float32)], axis=0).astype(jnp.bfloat16)

    def gathered(n):
        return jnp.concatenate([tab[t, n // side][:, n % side * pts:(n % side + 1) * pts] for t in range(cols)], axis=1)

    span = GROUP * rows
    lhs[...] = split(jnp.concatenate([gathered(n) for n in range(GROUP)], axis=0))

    def lanes(q):
        return pl.ds(pl.multiple_of(q * part, LANES), part)

    def push(left, accs, b, j, r):
        lam_t = jnp.concatenate([lam_ref[b, j, pl.ds(r + n, 1)] for n in range(2)], axis=1) * LOG2E
        cur_t = jnp.concatenate([curve[b, j, pl.ds(r + n, 1)] for n in range(2)], axis=1) * LOG2E
        c = consts[0]
        e = jnp.exp2(c * (lam_t + cur_t * c))
        ratio = jnp.exp2(wide * lam_t + cur_t * consts[1])
        turn = jnp.broadcast_to(jnp.exp2(cur_t * (2.0 * wide * wide)), e.shape)
        steps = DEPTH // STRIDE
        tiles = total_pts // DEPTH
        for n in range(tiles):
            highs, lows = [], []
            for m in range(steps):
                e_hi = e.astype(jnp.bfloat16)
                highs.append(e_hi)
                lows.append(e - e_hi.astype(jnp.float32))
                if n < tiles - 1 or m < steps - 1:
                    e = e * ratio
                    ratio = ratio * turn
            for q, pieces in enumerate((highs, lows)):
                pltpu.matmul_push_rhs(jnp.concatenate(pieces, axis=0), n % 2, q)
            piece = left[:, n * DEPTH:(n + 1) * DEPTH]
            for acc in accs:
                pltpu.matmul_acc_lhs(acc, piece, load_staged_rhs=n % 2)

    def pick(t):
        return (blocks - t) % 2

    def at_block(t):
        return pl.ds(t * 2 * LANES, 2 * LANES)

    def hand_on(b, j, q):
        at = species.at[b, j, :, lanes(q)]
        remote(at, at, psend.at[0], precv.at[0], col, partner).start()

    def member_copy(item, d, b, j, q):
        to = lax.rem(member + d, GROUP)
        return remote(stage.at[item, to], species.at[b, j, :, lanes(q)], msend.at[0], mrecv.at[item], group * GROUP + to, me)

    def member_arrivals(item):
        total_of(species.at[0, pl.ds(0, GROUP - 1), :, pl.ds(0, part)], msend.at[0], mrecv.at[item]).wait_recv()

    def y_copy(i, u, d, k):
        at = species.at[me, peer(u, d), :, lanes(PARTS - SINGLE + k)]
        return remote(at, at, ysend.at[0], yrecv.at[chips - 1 - i, u, k], col, other_chip(i))

    def y_arrivals(u, k):
        for i in range(1, chips):
            total_of(species.at[0, pl.ds(0, GROUP), :, pl.ds(0, part)], ysend.at[0], yrecv.at[i - 1, u, k]).wait_recv()

            @pl.loop(0, GROUP)
            def _(d):
                hand_on(other_chip(i), peer(u, d), PARTS - SINGLE + k)

    count = SINGLE + chips
    doubles_from = groups * count
    locals_from = doubles_from + groups * chips
    others = (GROUP - 1) * chips
    total = locals_from + groups * others
    spare = groups * per

    def place(n):
        u0, r0 = n // count, lax.rem(n, count)
        n1 = jnp.maximum(n - doubles_from, 0)
        u1, i1 = n1 // chips, lax.rem(n1, chips)
        n2 = jnp.maximum(n - locals_from, 0)
        u2, m2 = n2 // others, lax.rem(n2, others)
        single = jnp.logical_and(n < doubles_from, r0 < SINGLE)
        double = jnp.logical_and(n >= doubles_from, n < locals_from)
        late = n >= locals_from
        u = jnp.where(late, u2, jnp.where(double, u1, u0))
        i = jnp.where(late, lax.rem(m2, chips), jnp.where(double, i1, jnp.maximum(r0 - SINGLE, 0)))
        b = other_chip(i)
        j = peer(u, jnp.where(late, 1 + m2 // chips, 0))
        q = jnp.where(single, PARTS - SINGLE + r0, jnp.where(double, 1, 0))
        item = jnp.where(single, u * per + r0, jnp.where(double, u * per + SINGLE + i, spare))
        return single, u, r0, b, j, q, item

    def start(n, t):
        _, _, _, b, j, q, _ = place(n)
        push(lhs, sums[pick(t)], b, j, q * part_rows + t * 2)

    def done(n, t):
        item = place(n)[6]
        one, two = sums[pick(t)]
        acc = pltpu.matmul_pop(one) + pltpu.matmul_pop(two)
        inv = 1.0 / acc[2 * span:2 * span + 8]
        for g in range(GROUP):
            value = acc[g * rows:(g + 1) * rows] + acc[span + g * rows:span + (g + 1) * rows]
            stage[item, g, :, at_block(t)] = value * inv[:rows]

    def keep(n):
        _, _, _, b, j, q, item = place(n)
        species[b, j, :, lanes(q)] = stage[item, member]

    def sent(n):
        single, u, r, b, j, q, item = place(n)

        @pl.when(item < spare)
        def _():
            for d in range(1, GROUP):
                member_copy(item, d, b, j, q).start()

        @pl.when(single)
        def _():
            for i in range(1, chips):
                y_copy(i, u, 0, r).start()

        hand_on(b, j, q)

    def single_arrivals(u, k):
        member_arrivals(u * per + k)

        @pl.loop(1, GROUP)
        def _(d):
            for i in range(1, chips):
                y_copy(i, u, d, k).start()
            hand_on(me, peer(u, d), PARTS - SINGLE + k)

    def double_arrivals(u, i):
        member_arrivals(u * per + SINGLE + i)

        @pl.loop(1, GROUP)
        def _(d):
            hand_on(other_chip(i), peer(u, d), 1)

    def ready(n):
        @pl.when(n < doubles_from)
        def _():
            u, r = n // count, lax.rem(n, count)

            @pl.when(jnp.logical_and(r == 0, u > 0))
            def _():
                first_arrival(0, u).wait_recv()
                for d in range(1, GROUP):
                    second_copy(u, 0, d).start()

            @pl.when(r == SINGLE)
            def _():
                for i in range(1, chips):
                    first_arrival(i, u).wait_recv()
                    for d in range(1, GROUP):
                        second_copy(u, i, d).start()

                @pl.when(u == 0)
                def _():
                    total_of(curve.at[pl.ds(0, chips - 1), :, pl.ds(0, 2 * part_rows)], ksend.at[0], krecv.at[0]).wait_recv()

    def spread_two(e):
        for x in range(2):
            k = 2 * e + x
            second_arrival(k // (GROUP - 1), 1 + lax.rem(k, GROUP - 1)).wait_recv()

    def hand_on_lam(_):
        for i in range(chips):
            at = lam_ref.at[other_chip(i)]
            remote(at, at, lsend.at[0], lrecv.at[0], col, partner).start()

    doubles_pair, locals_pair, pairs = doubles_from // 2, locals_from // 2, total // 2
    events = (
        (doubles_pair + 1, 2, groups * (GROUP - 1) // 2, spread_two),
        (pairs - 2, 1, 1, hand_on_lam),
        *((doubles_pair + k, 3, groups, lambda u, k=k: single_arrivals(u, k)) for k in range(SINGLE)),
        (locals_pair + 3, 2, groups * SINGLE, lambda e: y_arrivals(e // SINGLE, lax.rem(e, SINGLE))),
        (locals_pair + 4, 1, groups * chips, lambda e: double_arrivals(e // chips, lax.rem(e, chips))),
    )

    def served(n):
        for begin, every, number, event in events:
            m = n - begin

            @pl.when(jnp.logical_and(jnp.logical_and(m >= 0, m < number * every), lax.rem(m, every) == 0))
            def _():
                event(m // every)

    @pl.loop(0, pairs)
    def _(p):
        ready(2 * p)
        for x in range(2):
            n = 2 * p + x
            back = n - 1 if x else jnp.maximum(n - 1, 0)
            for t in range(blocks):
                start(n, t)
                if t > 0:
                    done(n, t - 1)
                elif lag:
                    done(back, blocks - 1)
                    keep(back)
                    if x:
                        sent(back)
                    else:
                        @pl.when(p > 0)
                        def _():
                            sent(back)
            if not lag:
                done(n, blocks - 1)
                keep(n)
                sent(n)
        served(p)

    if lag:
        done(total - 1, blocks - 1)
        keep(total - 1)
        sent(total - 1)

    for begin, every, number, event in reversed(events):
        @pl.loop(max(0, min(number, -((begin - pairs) // every))), number)
        def _(e):
            event(e)


    total_of(tab.at[pl.ds(0, cols - 1)], tsend.at[0], trecv.at[0]).wait_send()
    total_of(curve.at[pl.ds(0, chips - 1), :, pl.ds(0, 2 * part_rows)], ksend.at[0], krecv.at[0]).wait_send()
    total_of(lam_ref.at[0, pl.ds(0, chips * groups - 1)], asend.at[0], lrecv.at[0]).wait_send()
    total_of(lam_ref.at[pl.ds(0, chips), pl.ds(0, (GROUP - 1) * groups)], bsend.at[0], lrecv.at[0]).wait_send()
    total_of(stage.at[pl.ds(0, spare), pl.ds(0, GROUP - 1)], msend.at[0], precv.at[0]).wait_send()
    total_of(species.at[pl.ds(0, chips - 1), :, :, pl.ds(0, SINGLE * part)], ysend.at[0], precv.at[0]).wait_send()
    total_of(lam_ref.at[pl.ds(0, chips)], lsend.at[0], lrecv.at[0]).wait()
    total_of(species.at[pl.ds(0, chips)], psend.at[0], precv.at[0]).wait()


def scoped_kernel(cols, bins, total_pts, rows, *refs):
    def pair(m):
        return tuple(pltpu.ACC(q)((m, 256), jnp.float32) for q in range(2))

    def body(sums):
        kernel(cols, bins, total_pts, rows, *refs, sums)

    m = 2 * GROUP * rows + 16
    pl.run_scoped(body, (pair(m), pair(m)))


def write_kernel(species, lam, out_ref, lam_out, sem):
    bins, cols, _, width = species.shape
    @pl.loop(0, bins)
    def _(b):
        for j in range(cols):
            to = pl.ds(pl.multiple_of((b * cols + j) * width, LANES), width)
            pltpu.make_async_copy(species.at[b, j], out_ref.at[:, to], sem.at[0]).start()

    keep = pltpu.make_async_copy(lam, lam_out, sem.at[1])
    keep.start()
    pltpu.make_async_copy(out_ref, out_ref, sem.at[0]).wait()
    keep.wait()


def per_device(slope, curvature, target_mean, target_var, table):
    cols = lax.axis_size("col")
    bins = lax.axis_size("bin")
    all_species, pts = table.shape
    rows = all_species // cols
    total_pts = pts * cols
    per_shard = slope.shape[0]
    sub = per_shard // cols // LANES
    width = sub * LANES
    chips = bins // 2
    groups = cols // GROUP
    items = groups * (SINGLE + chips)
    side = max(1, min(GROUP, LANES // pts))
    packed = (groups, GROUP // side, rows, side * pts)

    def blocks(a):
        return a.reshape(cols, sub, LANES)

    placed = table.reshape(cols, rows, pts)
    vmem = pl.BlockSpec(memory_space=pltpu.VMEM)
    hbm = pl.BlockSpec(memory_space=pltpu.HBM)
    dma = pltpu.SemaphoreType.DMA
    one = dma((1,))
    species, lam = pl.pallas_call(
        functools.partial(scoped_kernel, cols, bins, total_pts, rows),
        out_shape=(
            jax.ShapeDtypeStruct((bins, cols, rows, width), jnp.float32),
            jax.ShapeDtypeStruct((bins, cols, sub, LANES), jnp.float32),
        ),
        in_specs=[hbm] * 5,
        out_specs=(vmem, vmem),
        scratch_shapes=[
            pltpu.VMEM((3, sub, LANES), jnp.float32),
            pltpu.VMEM((bins, cols, sub, LANES), jnp.float32),
            pltpu.VMEM((cols, rows, pts), jnp.float32),
            pltpu.VMEM(packed, jnp.float32),
            pltpu.VMEM((cols, *packed[1:]), jnp.float32),
            pltpu.VMEM((2 * GROUP * rows + 16, total_pts), jnp.bfloat16),
            pltpu.VMEM((2, STRIDE, 2 * LANES), jnp.float32),
            pltpu.VMEM((items + 1, GROUP, rows, width // PARTS), jnp.float32),
            dma((5,)), pltpu.SemaphoreType.REGULAR,
            one, one, one, one, one, dma((chips, groups)),
            one, dma((groups, GROUP)),
            one, one, one, dma((items,)),
            one, dma((chips - 1, groups, SINGLE)), one, one,
        ],
        compiler_params=pltpu.CompilerParams(collective_id=0, has_side_effects=True, vmem_limit_bytes=24 << 20),
    )(*[
        pltpu.with_memory_space_constraint(a, pltpu.HBM)
        for a in (blocks(slope), blocks(curvature), blocks(target_mean), blocks(target_var), placed)
    ])
    species_mean, lam = pl.pallas_call(
        write_kernel,
        out_shape=(
            jax.ShapeDtypeStruct((rows, per_shard * bins), jnp.float32),
            jax.ShapeDtypeStruct((bins, cols, sub, LANES), jnp.float32),
        ),
        in_specs=[vmem, vmem],
        out_specs=(hbm, hbm),
        scratch_shapes=[dma((2,))],
        compiler_params=pltpu.CompilerParams(vmem_limit_bytes=4 << 20),
    )(species, lam)
    return species_mean, lam.reshape(-1)


def solution(mesh):
    placed = (P("bin"), P("bin"), P("bin"), P("bin"), P(None, "col"))
    return jax.shard_map(
        per_device, mesh=mesh, in_specs=placed, out_specs=(P("col", None), P()), check_vma=False
    )
```

```python
import functools
import math
import jax
import jax.numpy as jnp
from jax import lax
from jax.experimental import pallas as pl
from jax.experimental.pallas import tpu as pltpu
from jax.sharding import PartitionSpec as P

ITERS = 3
LANES = 128
LOG2E = math.log2(math.e)
MESH = pl.DeviceIdType.MESH
UNROLL = 32
STRIDE = 32
DEPTH = 256
GROUP = 4
RANK = 2
PARTS = 4
SINGLE = 2


def kernel(
    cols, bins, total_pts, rows,
    slope_hbm, curve_hbm, mean_hbm, var_hbm, placed_hbm,
    species, lam_ref,
    own, curve, placed, packed, tab, lhs, consts, stage,
    isem, far, tsend, trecv, ksend, krecv, asend, arecv, bsend, brecv,
    lsend, lrecv, msend, mrecv, ysend, yrecv, psend, precv,
    sums,
):
    col = lax.axis_index("col")
    me = lax.axis_index("bin")
    core = lax.rem(me, 2)
    partner = me + 1 - 2 * core
    chips = bins // 2
    groups = cols // GROUP
    member = lax.rem(col, GROUP)
    group = col // GROUP
    last = groups - 1
    sub = own.shape[1]
    width = sub * LANES
    part = width // PARTS
    part_rows = sub // PARTS
    pts = total_pts // cols
    side = packed.shape[3] // pts
    per = SINGLE + chips
    blocks = part_rows // 2
    lag = blocks % 2 == 0

    def other_chip(i):
        return lax.rem(me + 2 * i, bins)

    def peer(u, d):
        return lax.rem(group + u, groups) * GROUP + lax.rem(member + d, GROUP)

    def remote(src, dst, send, recv, c, b):
        return pltpu.make_async_remote_copy(
            src_ref=src, dst_ref=dst, send_sem=send, recv_sem=recv,
            device_id=(c, b), device_id_type=MESH,
        )

    def total_of(ref, send, recv):
        return remote(ref, ref, send, recv, col, partner)

    def greet(sem, c, b):
        pl.semaphore_signal(sem, inc=1, device_id=(c, b), device_id_type=MESH)

    barrier = pltpu.get_barrier_semaphore()
    rank = col // RANK
    ranks = cols // RANK

    def greet_rank(sem, k):
        for d in range(RANK):
            greet(sem, k * RANK + d, me)

    def greet_chips(sem, g):
        for i in range(1, chips):
            greet(sem, g * GROUP + member, other_chip(i))

    greet(barrier, col, partner)
    for d in range(1, RANK):
        greet(barrier, rank * RANK + lax.rem(col + d, RANK), me)

    @pl.loop(group, groups)
    def _(g):
        greet_chips(barrier, g)

    @pl.loop(rank + 1, ranks)
    def _(k):
        greet_rank(barrier, k)

    load_table = pltpu.make_async_copy(placed_hbm, placed, isem.at[4])
    load_table.start()
    loads = [
        pltpu.make_async_copy(a.at[col], own.at[n], isem.at[n])
        for n, a in enumerate((slope_hbm, mean_hbm, var_hbm))
    ]
    loads.append(pltpu.make_async_copy(curve_hbm, curve.at[me], isem.at[3]))
    for load in loads:
        load.start()

    for pair in sums:
        for acc in pair:
            pltpu.matmul_pop(acc)

    h = 1.0 / total_pts
    wide = STRIDE * h
    first = (lax.broadcasted_iota(jnp.int32, consts.shape[1:], 0).astype(jnp.float32) + 0.5) * h
    consts[0] = first
    consts[1] = wide * (2.0 * first + wide)

    load_table.wait()
    for g in range(groups):
        for p in range(GROUP // side):
            packed[g, p] = jnp.concatenate([placed[g * GROUP + p * side + n] for n in range(side)], axis=1)

    def table_copy(to):
        return remote(packed.at[to // GROUP], tab.at[col], tsend.at[0], trecv.at[0], to, me)

    def curve_copy(i):
        at = curve.at[me, :, pl.ds(0, 2 * part_rows)]
        return remote(at, at, ksend.at[0], krecv.at[0], col, other_chip(i))

    def enter():
        pl.semaphore_wait(barrier, (rank + 1) * RANK + (group + 1) * (chips - 1))

        @pl.loop(0, rank)
        def _(k):
            greet_rank(far, k)

        @pl.loop(0, group)
        def _(g):
            greet_chips(far, g)

        @pl.loop(0, rank)
        def _(k):
            for d in range(RANK):
                table_copy(k * RANK + d).start()

        for d in range(1, RANK):
            table_copy(rank * RANK + lax.rem(col + d, RANK)).start()
        tab[col] = packed[group]
        for i in range(1, chips):
            curve_copy(i).start()

    for load in loads:
        load.wait()

    @pl.when(rank > 0)
    def _():
        enter()

    curve2 = curve[me, col] * LOG2E
    target = own[1]
    var = own[2]
    bend = jnp.exp2(curve2 * (2.0 * h * h))

    def newton(lam):
        lam2 = lam * LOG2E

        def begin(g):
            c = ((g * UNROLL).astype(jnp.float32) + 0.5) * h
            return jnp.exp2(c * (lam2 + curve2 * c)), jnp.exp2(h * (lam2 + curve2 * (2.0 * c + h)))

        def body(g, carry):
            total, mom, e, ratio = carry
            later = begin(g + 1)
            c = ((g * UNROLL).astype(jnp.float32) + 0.5) * h
            run = e
            runs = e
            for i in range(1, UNROLL):
                e = e * ratio
                if i < UNROLL - 1:
                    ratio = ratio * bend
                run = run + e
                runs = runs + run
            return total + run, mom + (c * run + h * (UNROLL * run - runs)), *later

        zero = jnp.zeros_like(lam)
        total, mom, _, _ = lax.fori_loop(0, total_pts // UNROLL, body, (zero, zero, *begin(jnp.int32(0))))
        return lam + (target - mom / total) / var

    lam_ref[me, col] = lax.fori_loop(0, ITERS, lambda _, lam: newton(lam), own[0])

    @pl.when(rank == 0)
    def _():
        enter()

    def first_copy(i, u):
        at = lam_ref.at[me, col]
        return remote(at, at, asend.at[0], arecv.at[(chips - i) % chips, lax.rem(groups - u, groups)], peer(u, 0), other_chip(i))

    def first_arrival(i, u):
        b, j = other_chip(i), peer(u, 0)
        at = lam_ref.at[b, j]
        return remote(at, at, asend.at[0], arecv.at[i, u], j, b)

    def second_copy(u, i, d):
        at = lam_ref.at[other_chip(i), peer(u, 0)]
        return remote(at, at, bsend.at[0], brecv.at[u, member], peer(0, d), me)

    def second_arrival(u, d):
        at = lam_ref.at[pl.ds(0, chips), 0]
        return remote(at, at, bsend.at[0], brecv.at[u, lax.rem(member + d, GROUP)], col, partner)

    for i in range(1, chips):
        first_copy(i, 0).start()
    @pl.when(rank < ranks - 1)
    def _():
        pl.semaphore_wait(far, (ranks - 1 - rank) * RANK + (last - group) * (chips - 1))

        @pl.loop(rank + 1, ranks)
        def _(k):
            for d in range(RANK):
                table_copy(k * RANK + d).start()

    for d in range(1, GROUP):
        second_copy(0, 0, d).start()

    @pl.loop(1, groups)
    def _(u):
        for i in range(chips):
            first_copy(i, u).start()

    total_of(tab.at[pl.ds(0, cols - 1)], tsend.at[0], trecv.at[0]).wait_recv()

    def split(full):
        high = full.astype(jnp.bfloat16).astype(jnp.float32)
        return jnp.concatenate([high, full - high, jnp.ones((16, total_pts), jnp.float32)], axis=0).astype(jnp.bfloat16)

    def gathered(n):
        return jnp.concatenate([tab[t, n // side][:, n % side * pts:(n % side + 1) * pts] for t in range(cols)], axis=1)

    span = GROUP * rows
    lhs[...] = split(jnp.concatenate([gathered(n) for n in range(GROUP)], axis=0))

    def lanes(q):
        return pl.ds(pl.multiple_of(q * part, LANES), part)

    def push(left, accs, b, j, r):
        lam_t = jnp.concatenate([lam_ref[b, j, pl.ds(r + n, 1)] for n in range(2)], axis=1) * LOG2E
        cur_t = jnp.concatenate([curve[b, j, pl.ds(r + n, 1)] for n in range(2)], axis=1) * LOG2E
        c = consts[0]
        e = jnp.exp2(c * (lam_t + cur_t * c))
        ratio = jnp.exp2(wide * lam_t + cur_t * consts[1])
        turn = jnp.broadcast_to(jnp.exp2(cur_t * (2.0 * wide * wide)), e.shape)
        steps = DEPTH // STRIDE
        tiles = total_pts // DEPTH
        for n in range(tiles):
            highs, lows = [], []
            for m in range(steps):
                e_hi = e.astype(jnp.bfloat16)
                highs.append(e_hi)
                lows.append(e - e_hi.astype(jnp.float32))
                if n < tiles - 1 or m < steps - 1:
                    e = e * ratio
                    ratio = ratio * turn
            for q, pieces in enumerate((highs, lows)):
                pltpu.matmul_push_rhs(jnp.concatenate(pieces, axis=0), n % 2, q)
            piece = left[:, n * DEPTH:(n + 1) * DEPTH]
            for acc in accs:
                pltpu.matmul_acc_lhs(acc, piece, load_staged_rhs=n % 2)

    def pick(t):
        return (blocks - t) % 2

    def at_block(t):
        return pl.ds(t * 2 * LANES, 2 * LANES)

    def hand_on(b, j, q):
        at = species.at[b, j, :, lanes(q)]
        remote(at, at, psend.at[0], precv.at[0], col, partner).start()

    def member_copy(item, d, b, j, q):
        to = lax.rem(member + d, GROUP)
        return remote(stage.at[item, to], species.at[b, j, :, lanes(q)], msend.at[0], mrecv.at[item], group * GROUP + to, me)

    def member_arrivals(item):
        total_of(species.at[0, pl.ds(0, GROUP - 1), :, pl.ds(0, part)], msend.at[0], mrecv.at[item]).wait_recv()

    def y_copy(i, u, d, k):
        at = species.at[me, peer(u, d), :, lanes(PARTS - SINGLE + k)]
        return remote(at, at, ysend.at[0], yrecv.at[chips - 1 - i, u, k], col, other_chip(i))

    def y_arrivals(u, k):
        for i in range(1, chips):
            total_of(species.at[0, pl.ds(0, GROUP), :, pl.ds(0, part)], ysend.at[0], yrecv.at[i - 1, u, k]).wait_recv()

            @pl.loop(0, GROUP)
            def _(d):
                hand_on(other_chip(i), peer(u, d), PARTS - SINGLE + k)

    count = SINGLE + chips
    doubles_from = groups * count
    locals_from = doubles_from + groups * chips
    others = (GROUP - 1) * chips
    total = locals_from + groups * others
    spare = groups * per

    def place(n):
        u0, r0 = n // count, lax.rem(n, count)
        n1 = jnp.maximum(n - doubles_from, 0)
        u1, i1 = n1 // chips, lax.rem(n1, chips)
        n2 = jnp.maximum(n - locals_from, 0)
        u2, m2 = n2 // others, lax.rem(n2, others)
        single = jnp.logical_and(n < doubles_from, r0 < SINGLE)
        double = jnp.logical_and(n >= doubles_from, n < locals_from)
        late = n >= locals_from
        u = jnp.where(late, u2, jnp.where(double, u1, u0))
        i = jnp.where(late, lax.rem(m2, chips), jnp.where(double, i1, jnp.maximum(r0 - SINGLE, 0)))
        b = other_chip(i)
        j = peer(u, jnp.where(late, 1 + m2 // chips, 0))
        q = jnp.where(single, PARTS - SINGLE + r0, jnp.where(double, 1, 0))
        item = jnp.where(single, u * per + r0, jnp.where(double, u * per + SINGLE + i, spare))
        return single, u, r0, b, j, q, item

    def start(n, t):
        _, _, _, b, j, q, _ = place(n)
        push(lhs, sums[pick(t)], b, j, q * part_rows + t * 2)

    def done(n, t):
        item = place(n)[6]
        one, two = sums[pick(t)]
        acc = pltpu.matmul_pop(one) + pltpu.matmul_pop(two)
        inv = 1.0 / acc[2 * span:2 * span + 8]
        for g in range(GROUP):
            value = acc[g * rows:(g + 1) * rows] + acc[span + g * rows:span + (g + 1) * rows]
            stage[item, g, :, at_block(t)] = value * inv[:rows]

    def keep(n):
        _, _, _, b, j, q, item = place(n)
        species[b, j, :, lanes(q)] = stage[item, member]

    def sent(n):
        single, u, r, b, j, q, item = place(n)

        @pl.when(item < spare)
        def _():
            for d in range(1, GROUP):
                member_copy(item, d, b, j, q).start()

        @pl.when(single)
        def _():
            for i in range(1, chips):
                y_copy(i, u, 0, r).start()

        hand_on(b, j, q)

    def single_arrivals(u, k):
        member_arrivals(u * per + k)

        @pl.loop(1, GROUP)
        def _(d):
            for i in range(1, chips):
                y_copy(i, u, d, k).start()
            hand_on(me, peer(u, d), PARTS - SINGLE + k)

    def double_arrivals(u, i):
        member_arrivals(u * per + SINGLE + i)

        @pl.loop(1, GROUP)
        def _(d):
            hand_on(other_chip(i), peer(u, d), 1)

    def ready(n):
        @pl.when(n < doubles_from)
        def _():
            u, r = n // count, lax.rem(n, count)

            @pl.when(jnp.logical_and(r == 0, u > 0))
            def _():
                first_arrival(0, u).wait_recv()
                for d in range(1, GROUP):
                    second_copy(u, 0, d).start()

            @pl.when(r == SINGLE)
            def _():
                for i in range(1, chips):
                    first_arrival(i, u).wait_recv()
                    for d in range(1, GROUP):
                        second_copy(u, i, d).start()

                @pl.when(u == 0)
                def _():
                    total_of(curve.at[pl.ds(0, chips - 1), :, pl.ds(0, 2 * part_rows)], ksend.at[0], krecv.at[0]).wait_recv()

    def spread_two(e):
        for x in range(2):
            k = 2 * e + x
            second_arrival(k // (GROUP - 1), 1 + lax.rem(k, GROUP - 1)).wait_recv()

    def hand_on_lam(_):
        for i in range(chips):
            at = lam_ref.at[other_chip(i)]
            remote(at, at, lsend.at[0], lrecv.at[0], col, partner).start()

    doubles_pair, locals_pair, pairs = doubles_from // 2, locals_from // 2, total // 2
    events = (
        (doubles_pair + 1, 2, groups * (GROUP - 1) // 2, spread_two),
        (pairs - 2, 1, 1, hand_on_lam),
        *((doubles_pair + 2 * k, 3, groups, lambda u, k=k: single_arrivals(u, k)) for k in range(SINGLE)),
        (locals_pair + 3, 2, groups * SINGLE, lambda e: y_arrivals(e // SINGLE, lax.rem(e, SINGLE))),
        (locals_pair + 4, 1, groups * chips, lambda e: double_arrivals(e // chips, lax.rem(e, chips))),
    )

    def served(n):
        for begin, every, number, event in events:
            m = n - begin

            @pl.when(jnp.logical_and(jnp.logical_and(m >= 0, m < number * every), lax.rem(m, every) == 0))
            def _():
                event(m // every)

    @pl.loop(0, pairs)
    def _(p):
        ready(2 * p)
        for x in range(2):
            n = 2 * p + x
            back = n - 1 if x else jnp.maximum(n - 1, 0)
            for t in range(blocks):
                start(n, t)
                if t > 0:
                    done(n, t - 1)
                elif lag:
                    done(back, blocks - 1)
                    keep(back)
                    if x:
                        sent(back)
                    else:
                        @pl.when(p > 0)
                        def _():
                            sent(back)
            if not lag:
                done(n, blocks - 1)
                keep(n)
                sent(n)
        served(p)

    if lag:
        done(total - 1, blocks - 1)
        keep(total - 1)
        sent(total - 1)

    for begin, every, number, event in reversed(events):
        @pl.loop(max(0, min(number, -((begin - pairs) // every))), number)
        def _(e):
            event(e)


    total_of(tab.at[pl.ds(0, cols - 1)], tsend.at[0], trecv.at[0]).wait_send()
    total_of(curve.at[pl.ds(0, chips - 1), :, pl.ds(0, 2 * part_rows)], ksend.at[0], krecv.at[0]).wait_send()
    total_of(lam_ref.at[0, pl.ds(0, chips * groups - 1)], asend.at[0], lrecv.at[0]).wait_send()
    total_of(lam_ref.at[pl.ds(0, chips), pl.ds(0, (GROUP - 1) * groups)], bsend.at[0], lrecv.at[0]).wait_send()
    total_of(stage.at[pl.ds(0, spare), pl.ds(0, GROUP - 1)], msend.at[0], precv.at[0]).wait_send()
    total_of(species.at[pl.ds(0, chips - 1), :, :, pl.ds(0, SINGLE * part)], ysend.at[0], precv.at[0]).wait_send()
    total_of(lam_ref.at[pl.ds(0, chips)], lsend.at[0], lrecv.at[0]).wait()
    total_of(species.at[pl.ds(0, chips)], psend.at[0], precv.at[0]).wait()


def scoped_kernel(cols, bins, total_pts, rows, *refs):
    def pair(m):
        return tuple(pltpu.ACC(q)((m, 256), jnp.float32) for q in range(2))

    def body(sums):
        kernel(cols, bins, total_pts, rows, *refs, sums)

    m = 2 * GROUP * rows + 16
    pl.run_scoped(body, (pair(m), pair(m)))


def write_kernel(species, lam, out_ref, lam_out, sem):
    bins, cols, _, width = species.shape
    @pl.loop(0, bins)
    def _(b):
        for j in range(cols):
            to = pl.ds(pl.multiple_of((b * cols + j) * width, LANES), width)
            pltpu.make_async_copy(species.at[b, j], out_ref.at[:, to], sem.at[0]).start()

    keep = pltpu.make_async_copy(lam, lam_out, sem.at[1])
    keep.start()
    pltpu.make_async_copy(out_ref, out_ref, sem.at[0]).wait()
    keep.wait()


def per_device(slope, curvature, target_mean, target_var, table):
    cols = lax.axis_size("col")
    bins = lax.axis_size("bin")
    all_species, pts = table.shape
    rows = all_species // cols
    total_pts = pts * cols
    per_shard = slope.shape[0]
    sub = per_shard // cols // LANES
    width = sub * LANES
    chips = bins // 2
    groups = cols // GROUP
    items = groups * (SINGLE + chips)
    side = max(1, min(GROUP, LANES // pts))
    packed = (groups, GROUP // side, rows, side * pts)

    def blocks(a):
        return a.reshape(cols, sub, LANES)

    placed = table.reshape(cols, rows, pts)
    vmem = pl.BlockSpec(memory_space=pltpu.VMEM)
    hbm = pl.BlockSpec(memory_space=pltpu.HBM)
    dma = pltpu.SemaphoreType.DMA
    one = dma((1,))
    species, lam = pl.pallas_call(
        functools.partial(scoped_kernel, cols, bins, total_pts, rows),
        out_shape=(
            jax.ShapeDtypeStruct((bins, cols, rows, width), jnp.float32),
            jax.ShapeDtypeStruct((bins, cols, sub, LANES), jnp.float32),
        ),
        in_specs=[hbm] * 5,
        out_specs=(vmem, vmem),
        scratch_shapes=[
            pltpu.VMEM((3, sub, LANES), jnp.float32),
            pltpu.VMEM((bins, cols, sub, LANES), jnp.float32),
            pltpu.VMEM((cols, rows, pts), jnp.float32),
            pltpu.VMEM(packed, jnp.float32),
            pltpu.VMEM((cols, *packed[1:]), jnp.float32),
            pltpu.VMEM((2 * GROUP * rows + 16, total_pts), jnp.bfloat16),
            pltpu.VMEM((2, STRIDE, 2 * LANES), jnp.float32),
            pltpu.VMEM((items + 1, GROUP, rows, width // PARTS), jnp.float32),
            dma((5,)), pltpu.SemaphoreType.REGULAR,
            one, one, one, one, one, dma((chips, groups)),
            one, dma((groups, GROUP)),
            one, one, one, dma((items,)),
            one, dma((chips - 1, groups, SINGLE)), one, one,
        ],
        compiler_params=pltpu.CompilerParams(collective_id=0, has_side_effects=True, vmem_limit_bytes=24 << 20),
    )(*[
        pltpu.with_memory_space_constraint(a, pltpu.HBM)
        for a in (blocks(slope), blocks(curvature), blocks(target_mean), blocks(target_var), placed)
    ])
    species_mean, lam = pl.pallas_call(
        write_kernel,
        out_shape=(
            jax.ShapeDtypeStruct((rows, per_shard * bins), jnp.float32),
            jax.ShapeDtypeStruct((bins, cols, sub, LANES), jnp.float32),
        ),
        in_specs=[vmem, vmem],
        out_specs=(hbm, hbm),
        scratch_shapes=[dma((2,))],
        compiler_params=pltpu.CompilerParams(vmem_limit_bytes=4 << 20),
    )(species, lam)
    return species_mean, lam.reshape(-1)


def solution(mesh):
    placed = (P("bin"), P("bin"), P("bin"), P("bin"), P(None, "col"))
    return jax.shard_map(
        per_device, mesh=mesh, in_specs=placed, out_specs=(P("col", None), P()), check_vma=False
    )
```
